32 devices in a mesh: member: 8 (over y, x, core), region: 4 (over z).
Axes of the slice: x: 2, y: 2, z: 4, core: 2. Of those that a mesh axis runs over, the one named last changes fastest.
Arguments:
- prior_sample_matrix: float32 [128, 65536], P(('member', 'region')), may hold values from -18 to 18
- obs_values: float32 [1024], replicated, may hold values from -18 to 18
- obs_var: float32 [1024], replicated, may hold values from 0.5 to 4
- measured_indexes: int32 [1024], replicated, may hold values from 0 to 65535
- neighbours: int32 [128, 128], replicated, may hold values from 0 to 1023, as said below
- perturbation: float32 [128, 1024], P(('member', 'region')), may hold values from -6 to 6
- counts: int32 [32], replicated, may hold values from 1 to 8, as said below
Outputs:
- owned: float32 [256, 65536], P(('member', 'region'))
The draws below stay inside these ranges and needn't reach their ends.
Inputs may be any that keep to these rules, and one draw needn't show every extreme that they name: `neighbours`: each row lists 128 different observations. The counts sum to 128; some device owns exactly 8; the exclusive prefix sum of counts at device d differs from d * 4 by at most 2.
All inputs are finite; a program needn't handle non-finite values.
Results may differ from the reference program's by a relative error of at most 0.0003.
Values sent between devices are 32-bit elements; how exact they have to be, the bound alone decides.
No kernel may reach another device: no remote copies, remote signals or barrier semaphores. Data moves between devices by JAX's collectives and lax.ppermute only.
A program may use at most 128 MiB of HBM per device.

```python
import math
import jax
import jax.numpy as jnp
from jax import lax

S = 65536
NOBS = 1024
LOC = 128
ZONE_GRIDPOINTS = 512
PREDICT_SUBTICKS = 24
MEM_DEV = 4
M = 128
CAP = 8
REGIONS = 128
LSCALE = 2048
DEVICES = 32


def place_observations(key):
    return jax.random.randint(jax.random.fold_in(key, 11), (NOBS,), 0, S, dtype=jnp.int32)


def draw_measured_indexes(key, part):
    return place_observations(key)


def draw_neighbours(key, part):
    places = place_observations(key)
    centre = jnp.arange(REGIONS, dtype=jnp.int32) * ZONE_GRIDPOINTS + ZONE_GRIDPOINTS // 2
    gap_raw = jnp.abs(places[None, :] - centre[:, None])
    distance = jnp.minimum(gap_raw, S - gap_raw)
    scores = distance * NOBS + jnp.arange(NOBS, dtype=jnp.int32)[None, :]
    ordering = jnp.argsort(scores, axis=1, stable=True)
    return ordering[:, :LOC].astype(jnp.int32)


def draw_counts(key, part):
    half = MEM_DEV // 2
    drift = jax.random.randint(jax.random.fold_in(key, 21), (DEVICES + 1,), 1 - half, half, dtype=jnp.int32)
    places = jnp.arange(DEVICES + 1, dtype=jnp.int32)
    spot = jax.random.randint(jax.random.fold_in(key, 22), (), 1, DEVICES - 1, dtype=jnp.int32)
    drift = jnp.where(places == spot, -half, drift)
    drift = jnp.where(places == spot + 1, half, drift)
    drift = jnp.where((places == 0) | (places == DEVICES), 0, drift)
    offsets = places * MEM_DEV + drift
    return (offsets[1:] - offsets[:-1]).astype(jnp.int32)


def block_scale(own_key, extent, cuts, low, high):
    def one(position, blocks):
        steps = jax.random.uniform(jax.random.fold_in(jax.random.fold_in(own_key, 6), position), (blocks,), jnp.float32, low / len(cuts), high / len(cuts))
        return jnp.repeat(jnp.exp(steps), extent[position] // blocks).reshape((-1,) + (1,) * (len(extent) - position - 1))

    gain = one(*cuts[0])
    for cut in cuts[1:]:
        gain = gain * one(*cut)
    return gain


def centred(stream_key, extent, scale, reach, shards=(), kind=jnp.bfloat16):
    loudness = block_scale(stream_key, extent, shards, -0.22, 0.18) if shards else 1.0
    entries = jax.random.normal(stream_key, extent, jnp.float32) * scale * loudness
    return jnp.minimum(jnp.maximum(entries, -reach), reach).astype(kind)


def setup_inputs(seed: int = 0) -> dict:
    splits = jax.random.split(jax.random.key(seed), 8)
    prior_sample_matrix = centred(splits[0], (M, S), 3.0, 18.0, ((0, 32),), jnp.float32)
    obs_values = centred(splits[1], (NOBS,), 3.0, 18.0, (), jnp.float32)
    obs_var = jnp.clip(jnp.exp(jax.random.uniform(splits[2], (NOBS,), jnp.float32, math.log(0.5), math.log(4.0))), 0.5, 4.0)
    measured_indexes = draw_measured_indexes(jax.random.fold_in(splits[7], 71), 0)
    neighbours = draw_neighbours(jax.random.fold_in(splits[7], 71), 0)
    perturbation = centred(splits[5], (M, NOBS), 1.0, 6.0, ((0, 32),), jnp.float32)
    counts = draw_counts(jax.random.fold_in(splits[7], 71), 0)
    return dict(prior_sample_matrix=prior_sample_matrix, obs_values=obs_values, obs_var=obs_var, measured_indexes=measured_indexes, neighbours=neighbours, perturbation=perturbation, counts=counts)


FORCING = 8.0
TIME_STEP = 0.01
HIGH = lax.Precision.HIGHEST

def propagate_dynamics(lorenz_vector):
    tendency = (jnp.roll(lorenz_vector, -1, axis=1) - jnp.roll(lorenz_vector, 2, axis=1)) * jnp.roll(lorenz_vector, 1, axis=1) - lorenz_vector + FORCING
    return lorenz_vector + TIME_STEP * tendency

def obs_error(zone_identifier, columns, obs_var, measured_indexes):
    centre = zone_identifier * ZONE_GRIDPOINTS + ZONE_GRIDPOINTS // 2
    gap_raw = jnp.abs(measured_indexes[columns] - centre)
    distance = jnp.minimum(gap_raw, S - gap_raw).astype(jnp.float32)
    scaled = distance / float(LSCALE)
    return obs_var[columns] * (1.0 + scaled * scaled)

def analyse(zone_gridpoint_matrix, obs_raw, innov_cols, errors):
    divisor = float(zone_gridpoint_matrix.shape[0] - 1)
    anomalies = zone_gridpoint_matrix - lax.optimization_barrier(jnp.mean(zone_gridpoint_matrix, axis=0, keepdims=True))
    obs_anom = obs_raw - lax.optimization_barrier(jnp.mean(obs_raw, axis=0, keepdims=True))
    obs_cov = jnp.dot(obs_anom.T.astype(jnp.float32), obs_anom.astype(jnp.float32), precision=HIGH, preferred_element_type=jnp.float32) / divisor + jnp.diag(errors)
    factor = jnp.linalg.cholesky(obs_cov)
    solved = jax.scipy.linalg.cho_solve((factor, True), innov_cols.T)
    regression = jnp.dot(obs_anom.T.astype(jnp.float32), anomalies.astype(jnp.float32), precision=HIGH, preferred_element_type=jnp.float32) / divisor
    return zone_gridpoint_matrix + jnp.dot(solved.T.astype(jnp.float32), regression.astype(jnp.float32), precision=HIGH, preferred_element_type=jnp.float32)

def reference(prior_sample_matrix, obs_values, obs_var, measured_indexes, neighbours, perturbation, counts):
    predict_trajectory = lax.fori_loop(0, PREDICT_SUBTICKS, lambda single_subtick, lorenz_vector: propagate_dynamics(lorenz_vector), prior_sample_matrix)
    predicted_readings = predict_trajectory[:, measured_indexes]
    innovation = obs_values[None, :] + jnp.sqrt(obs_var)[None, :] * perturbation - predicted_readings

    def one_region(zone_identifier):
        columns = neighbours[zone_identifier]
        zone_gridpoint_matrix = lax.dynamic_slice_in_dim(predict_trajectory, (zone_identifier * ZONE_GRIDPOINTS).astype(jnp.int32), ZONE_GRIDPOINTS, 1)
        return analyse(zone_gridpoint_matrix, predicted_readings[:, columns], innovation[:, columns], obs_error(zone_identifier, columns, obs_var, measured_indexes))
    blocks = lax.map(one_region, jnp.arange(REGIONS, dtype=jnp.int32))
    sample_total = predict_trajectory.shape[0]
    analysed = jnp.transpose(blocks, (1, 0, 2)).reshape(sample_total, S)
    stepped = propagate_dynamics(analysed)
    offsets = jnp.cumsum(counts) - counts
    slot_index = jnp.arange(CAP, dtype=jnp.int32)
    member_index = offsets[:, None] + slot_index[None, :]
    occupied = slot_index[None, :] < counts[:, None]
    picked = jnp.where(occupied, member_index, 0).reshape(-1).astype(jnp.int32)
    owned_rows = stepped[picked]
    return jnp.where(occupied.reshape(-1)[:, None], owned_rows, 0.0)
```

```python
import functools

import jax
import jax.numpy as jnp
from jax import lax
from jax.experimental import pallas as pl
from jax.experimental.pallas import tpu as pltpu
from jax.sharding import PartitionSpec as P

PREDICT_SUBTICKS = 24
CAP = 8
LSCALE = 2048
FORCING = 8.0
TIME_STEP = 0.01
HIGH = lax.Precision.HIGHEST
AXES = ("member", "region")
LANES = 128
ROWS = 8


def lanes_iota():
    return lax.broadcasted_iota(jnp.int32, (ROWS, LANES), 1)


def rows_iota():
    return lax.broadcasted_iota(jnp.int32, (ROWS, LANES), 0)


def forecast_kernel(slot_ref, turn_ref, part_ref, x_ref, state_ref, readings_ref, *, devices, members):
    parts = ROWS // members
    steps = state_ref.shape[0] // devices // ROWS
    total = devices * steps
    lane = lanes_iota()
    row = rows_iota()
    first_lane = lane == 0
    low_lanes = lane < 2
    last_lane = lane == LANES - 1
    first_part = row < members
    last_part = row >= ROWS - members

    for destination in range(devices):
        for part in range(parts):
            for step in range(steps):
                tile = (destination * parts + part) * steps + step
                begin = (destination * steps + step) * ROWS + part * members
                state_ref[begin : begin + members, :] = x_ref[:, tile * LANES : (tile + 1) * LANES] * TIME_STEP

    def load(number):
        return state_ref[number * ROWS : (number + 1) * ROWS, :]

    def substep(_, carry):
        wrap_first = pltpu.roll(load(0), ROWS - members, axis=0)
        below = pltpu.roll(load(total - 1), members, axis=0)
        for destination in range(devices):
            start = destination * steps
            own_last = pltpu.roll(load(start + steps - 1), members, axis=0)
            previous = jnp.where(first_part, below, own_last)
            below = own_last
            if destination == 0:
                own_first = wrap_first
            else:
                own_first = next_first
            if destination + 1 < devices:
                next_first = pltpu.roll(load(start + steps), ROWS - members, axis=0)
            else:
                next_first = wrap_first
            following = jnp.where(last_part, next_first, own_first)
            previous_one = pltpu.roll(previous, 1, axis=1)
            previous_two = pltpu.roll(previous, 2, axis=1)
            current = load(start)
            current_up = pltpu.roll(current, LANES - 1, axis=1)
            for step in range(steps):
                after = load(start + step + 1) if step + 1 < steps else following
                after_up = pltpu.roll(after, LANES - 1, axis=1)
                one = pltpu.roll(current, 1, axis=1)
                two = pltpu.roll(current, 2, axis=1)
                left = jnp.where(first_lane, previous_one, one)
                left_two = jnp.where(low_lanes, previous_two, two)
                right = jnp.where(last_lane, after_up, current_up)
                updated = (current * (1.0 - TIME_STEP) + FORCING * TIME_STEP * TIME_STEP) + (right - left_two) * left
                begin = (start + step) * ROWS
                state_ref[begin : begin + ROWS, :] = updated
                previous_one, previous_two = one, two
                current, current_up = after, after_up
        return carry

    lax.fori_loop(0, PREDICT_SUBTICKS, substep, 0)

    for number in range(total):
        begin = number * ROWS
        state_ref[begin : begin + ROWS, :] = load(number) * (1.0 / TIME_STEP)

    def gather(block, carry):
        base = block * LANES
        picked = [jnp.zeros((ROWS, LANES), jnp.float32) for _ in range(4)]
        for number in range(LANES):
            begin = pl.multiple_of(slot_ref[base + number] * ROWS, ROWS)
            turned = pltpu.roll(state_ref[pl.ds(begin, ROWS), :], turn_ref[base + number], axis=1)
            picked[number % 4] = jnp.where(lane == number, turned, picked[number % 4])
        both = picked[0]
        for number in range(1, 4):
            both = jnp.where(lane % 4 == number, picked[number], both)
        part_of = part_ref[pl.ds(block, 1), :]
        chosen = both
        for part in range(1, parts):
            chosen = jnp.where(part_of == part, pltpu.roll(both, ROWS - part * members, axis=0), chosen)
        for destination in range(devices):
            readings_ref[destination, pl.ds(block * members, members), :] = chosen[:members]
        return carry

    lax.fori_loop(0, part_ref.shape[0], gather, 0)


def dot(a, b, contract, precision=HIGH):
    return lax.dot_general(a, b, (contract, ((), ())), precision=precision, preferred_element_type=jnp.float32)


def invert_all(matrix_ref):
    regions, size, _ = matrix_ref.shape
    lane = lanes_iota()
    row = rows_iota()

    def column(value, index):
        return jnp.take_along_axis(value, jnp.full((ROWS, LANES), index, jnp.int32), axis=1)

    def panel(number, carry):
        base = number * ROWS
        start = pl.multiple_of(base, ROWS)
        inside = (lane >= base) & (lane < base + ROWS)
        unit = jnp.where(lane - base == row, 1.0, 0.0)
        finished = []
        for region in range(regions):
            block = matrix_ref[region, pl.ds(start, ROWS), :]
            columns = [column(block, base + k) for k in range(ROWS)]
            block = jnp.where(inside, unit, block)
            for j in range(ROWS):
                inverse = 1.0 / columns[j][j : j + 1, :]
                here = row == j
                scaled = block[j : j + 1, :] * inverse
                block = jnp.where(here, scaled, block - columns[j] * scaled)
                for k in range(j + 1, ROWS):
                    scaled = columns[k][j : j + 1, :] * inverse
                    columns[k] = jnp.where(here, scaled, columns[k] - columns[j] * scaled)
            finished.append(block)
        for region in range(regions):
            block = finished[region]
            for i in range(size // ROWS):
                other = matrix_ref[region, i * ROWS : (i + 1) * ROWS, :]
                result = jnp.where(inside, 0.0, other)
                for k in range(ROWS):
                    result = result - column(other, base + k) * block[k : k + 1, :]
                matrix_ref[region, i * ROWS : (i + 1) * ROWS, :] = result
            matrix_ref[region, pl.ds(start, ROWS), :] = block
        return carry

    lax.fori_loop(0, size // ROWS, panel, 0)


def solve_kernel(
    zone_ref, neighbours_ref, table_ref, readings_ref, noise_ref, transform_ref, stack_ref, pieces_ref, matrix_ref, *, cells, zone_cells
):
    devices, _, _ = readings_ref.shape
    regions, total, _ = transform_ref.shape
    members = total // devices
    observations = table_ref.shape[1]
    extra = stack_ref.shape[0] - 2 * total
    for block in range(observations // LANES):
        lanes = slice(block * LANES, (block + 1) * LANES)
        values = table_ref[0:1, lanes]
        spread = jnp.sqrt(table_ref[1:2, lanes])
        for source in range(devices):
            equivalents = readings_ref[source, block * members : (block + 1) * members, :]
            noise = noise_ref[source, block * members : (block + 1) * members, :]
            stack_ref[source * members : (source + 1) * members, lanes] = equivalents
            stack_ref[total + source * members : total + (source + 1) * members, lanes] = values + spread * noise - equivalents
    stack_ref[2 * total : 2 * total + ROWS, :] = table_ref[...]
    stack_ref[2 * total + ROWS :, :] = jnp.zeros((extra - ROWS, observations), jnp.float32)
    height = stack_ref.shape[0]
    rest = stack_ref[...]
    for piece in range(3):
        rounded = rest.astype(jnp.bfloat16)
        pieces_ref[piece * height : (piece + 1) * height, :] = rounded
        rest = rest - rounded.astype(jnp.float32)

    centre0 = zone_ref[0] * zone_cells + zone_cells // 2
    size = neighbours_ref.shape[1]
    diagonal = lax.broadcasted_iota(jnp.int32, (size, size), 0) == lax.broadcasted_iota(jnp.int32, (size, size), 1)
    ids = lax.broadcasted_iota(jnp.int32, (observations, size), 0)
    anomalies, innovations = [], []
    for region in range(regions):
        pick = jnp.where(ids == neighbours_ref[region : region + 1, :], 1.0, 0.0).astype(jnp.bfloat16)
        picked = dot(pieces_ref[...], pick, ((1,), (0,)), lax.Precision.DEFAULT)
        picked = picked[:height] + picked[height : 2 * height] + picked[2 * height :]
        equivalents = picked[:total]
        innovations.append(picked[total : 2 * total])
        variance = picked[2 * total + 1 : 2 * total + 2]
        place = picked[2 * total + 2 : 2 * total + 3]
        centre = (centre0 + region * zone_cells).astype(jnp.float32)
        gap = jnp.abs(place - centre)
        scaled = jnp.minimum(gap, cells - gap) / float(LSCALE)
        errors = variance * (1.0 + scaled * scaled)
        anomaly = equivalents - jnp.sum(equivalents, axis=0, keepdims=True) * (1.0 / total)
        anomalies.append(anomaly)
        covariance = dot(anomaly, anomaly, ((0,), (0,))) * (1.0 / (total - 1))
        matrix_ref[region, :, :] = jnp.where(diagonal, covariance + errors, covariance)
    invert_all(matrix_ref)
    for region in range(regions):
        weights = dot(innovations[region], matrix_ref[region], ((1,), (0,)))
        transform_ref[region, :, :] = dot(weights, anomalies[region], ((1,), (1,))) * (1.0 / (total - 1))


def apply_kernel(counts_ref, transform_ref, cells_ref, owned_ref, block_ref, result_ref):
    sources, height, _ = cells_ref.shape
    regions, total, _ = transform_ref.shape
    members = total // sources
    parts = ROWS // members
    steps = height // ROWS
    tiles = parts * steps
    wide = tiles // regions
    for part in range(parts):
        for step in range(steps):
            tile = part * steps + step
            region, place = tile // wide, tile % wide
            begin = step * ROWS + part * members
            for source in range(sources):
                block_ref[region, source * members : (source + 1) * members, place * LANES : (place + 1) * LANES] = cells_ref[
                    source, begin : begin + members, :
                ]
    for region in range(regions):
        block = block_ref[region]
        anomalies = block - jnp.sum(block, axis=0, keepdims=True) * (1.0 / total)
        analysed = block + dot(transform_ref[region], anomalies, ((1,), (0,)))
        for place in range(wide):
            result_ref[region * wide + place, :total, :] = analysed[:, place * LANES : (place + 1) * LANES]
    for tile in range(tiles):
        result_ref[tile, total:, :] = jnp.zeros((ROWS, LANES), jnp.float32)

    def window(destination, offset):
        for tile in range(tiles):
            owned_ref[destination, tile * ROWS : (tile + 1) * ROWS, :] = result_ref[tile, pl.ds(offset, CAP), :]
        return offset + counts_ref[destination]

    lax.fori_loop(0, sources, window, jnp.int32(0))


def advance_kernel(count_ref, rows_ref, out_ref):
    tiles = rows_ref.shape[0] // ROWS
    here = out_ref.shape[1] // LANES
    lane = lanes_iota()
    occupied = rows_iota() < count_ref[0]
    start = pl.program_id(0) * here

    def load(number):
        return rows_ref[pl.ds(pl.multiple_of(number * ROWS, ROWS), ROWS), :]

    before = load(lax.rem(start + tiles - 1, tiles))
    before_one = pltpu.roll(before, 1, axis=1)
    before_two = pltpu.roll(before, 2, axis=1)
    current = load(start)
    current_up = pltpu.roll(current, LANES - 1, axis=1)
    for tile in range(here):
        after = load(start + tile + 1) if tile + 1 < here else load(lax.rem(start + here, tiles))
        after_up = pltpu.roll(after, LANES - 1, axis=1)
        one = pltpu.roll(current, 1, axis=1)
        two = pltpu.roll(current, 2, axis=1)
        left = jnp.where(lane == 0, before_one, one)
        left_two = jnp.where(lane < 2, before_two, two)
        right = jnp.where(lane == LANES - 1, after_up, current_up)
        stepped = current + TIME_STEP * ((right - left_two) * left - current + FORCING)
        out_ref[:, tile * LANES : (tile + 1) * LANES] = jnp.where(occupied, stepped, 0.0)
        before_one, before_two = one, two
        current, current_up = after, after_up


def whole(space=pltpu.VMEM):
    return pl.BlockSpec(memory_space=space)


def per_device(prior_sample_matrix, obs_values, obs_var, measured_indexes, neighbours, perturbation, counts):
    devices = lax.axis_size(AXES)
    device_index = lax.axis_index(AXES)
    members, cells = prior_sample_matrix.shape
    total = members * devices
    observations = obs_values.shape[0]
    zones, local = neighbours.shape
    regions = zones // devices
    zone_cells = cells // zones
    parts = ROWS // members
    share = cells // devices
    steps = share // LANES // parts
    blocks = observations // LANES

    slot = (measured_indexes // share) * steps + (measured_indexes // LANES) % steps
    part = (measured_indexes // (LANES * steps)) % parts
    turn = (jnp.arange(observations, dtype=jnp.int32) - measured_indexes) % LANES
    state, readings = pl.pallas_call(
        functools.partial(forecast_kernel, devices=devices, members=members),
        out_shape=(
            jax.ShapeDtypeStruct((devices * steps * ROWS, LANES), jnp.float32),
            jax.ShapeDtypeStruct((devices, blocks * members, LANES), jnp.float32),
        ),
        in_specs=[whole(pltpu.SMEM), whole(pltpu.SMEM), whole(), whole()],
        out_specs=(whole(), whole()),
        name="forecast",
    )(slot, turn, part.reshape(blocks, LANES), prior_sample_matrix)

    noise = perturbation.reshape(members, blocks, LANES).transpose(1, 0, 2).reshape(1, blocks * members, LANES)
    exchange = functools.partial(lax.all_to_all, axis_name=AXES, split_axis=0, concat_axis=0, tiled=True)
    noise = exchange(jnp.broadcast_to(noise, (devices, blocks * members, LANES)))
    readings = exchange(readings)
    own_cells = exchange(state.reshape(devices, steps * ROWS, LANES))

    zone = device_index * regions
    table = jnp.stack([obs_values, obs_var, measured_indexes.astype(jnp.float32)])
    table = jnp.concatenate([table, jnp.zeros((ROWS - 3, observations), jnp.float32)])
    height = 2 * total + 2 * ROWS
    transform = pl.pallas_call(
        functools.partial(solve_kernel, cells=float(cells), zone_cells=zone_cells),
        out_shape=jax.ShapeDtypeStruct((regions, total, total), jnp.float32),
        in_specs=[whole(pltpu.SMEM), whole(), whole(), whole(), whole()],
        out_specs=whole(),
        scratch_shapes=[
            pltpu.VMEM((height, observations), jnp.float32),
            pltpu.VMEM((3 * height, observations), jnp.bfloat16),
            pltpu.VMEM((regions, local, local), jnp.float32),
        ],
        name="solve",
    )(zone.reshape(1), lax.dynamic_slice_in_dim(neighbours, zone, regions, 0), table, readings, noise)

    tiles = share // LANES
    outgoing = pl.pallas_call(
        apply_kernel,
        out_shape=jax.ShapeDtypeStruct((devices, tiles * CAP, LANES), jnp.float32),
        in_specs=[whole(pltpu.SMEM), whole(), whole()],
        out_specs=whole(),
        scratch_shapes=[
            pltpu.VMEM((regions, total, zone_cells), jnp.float32),
            pltpu.VMEM((tiles, total + ROWS, LANES), jnp.float32),
        ],
        name="analyse",
    )(counts, transform, own_cells)
    owned = exchange(outgoing).reshape(devices * tiles * CAP, LANES)

    chunks = 8
    return pl.pallas_call(
        advance_kernel,
        grid=(chunks,),
        out_shape=jax.ShapeDtypeStruct((CAP, cells), jnp.float32),
        in_specs=[whole(pltpu.SMEM), whole()],
        out_specs=pl.BlockSpec((CAP, cells // chunks), lambda i: (0, i)),
        name="advance",
    )(lax.dynamic_slice_in_dim(counts, device_index, 1, 0), owned)


def solution(mesh):
    rows = P(AXES, None)
    return jax.shard_map(
        per_device, mesh=mesh, in_specs=(rows, P(), P(), P(), P(), rows, P()), out_specs=rows, check_vma=False
    )
```

```python
import functools

import jax
import jax.numpy as jnp
from jax import lax
from jax.experimental import pallas as pl
from jax.experimental.pallas import tpu as pltpu
from jax.sharding import PartitionSpec as P

PREDICT_SUBTICKS = 24
CAP = 8
LSCALE = 2048
FORCING = 8.0
TIME_STEP = 0.01
HIGH = lax.Precision.HIGHEST
AXES = ("member", "region")
LANES = 128
ROWS = 8


def lanes_iota():
    return lax.broadcasted_iota(jnp.int32, (ROWS, LANES), 1)


def rows_iota():
    return lax.broadcasted_iota(jnp.int32, (ROWS, LANES), 0)


def forecast_kernel(places_ref, runs_ref, x_ref, state_ref, readings_ref, tile_ref, *, devices, members):
    height = x_ref.shape[0]
    tiles = height // LANES
    halves = tiles // ROWS
    tile_pitch = LANES + ROWS
    cell_pitch = tiles + ROWS
    parts = ROWS // members
    lane = lanes_iota()
    row = rows_iota()

    def group(cell):
        return [state_ref[cell * tiles + half * ROWS : cell * tiles + (half + 1) * ROWS, :] for half in range(halves)]

    for tile in range(tiles):
        tile_ref[tile * tile_pitch : tile * tile_pitch + LANES, :] = (x_ref[tile * LANES : (tile + 1) * LANES, :] * TIME_STEP).T
    for cell in range(LANES):
        for half in range(halves):
            begin = cell * tiles + half * ROWS
            state_ref[begin : begin + ROWS, :] = tile_ref[pl.ds(half * ROWS * tile_pitch + cell, ROWS, stride=tile_pitch), :]

    def next_run(values):
        turned = [pltpu.roll(value, LANES - members, axis=1) for value in values]
        down = [pltpu.roll(value, ROWS - 1, axis=0) for value in turned]
        carried = [jnp.where(row == ROWS - 1, down[(half + 1) % halves], down[half]) for half in range(halves)]
        return [jnp.where(lane >= LANES - members, carry, value) for carry, value in zip(carried, turned, strict=True)]

    def previous_run(values):
        turned = [pltpu.roll(value, members, axis=1) for value in values]
        up = [pltpu.roll(value, 1, axis=0) for value in turned]
        carried = [jnp.where(row == 0, up[half - 1], up[half]) for half in range(halves)]
        return [jnp.where(lane < members, carry, value) for carry, value in zip(carried, turned, strict=True)]

    def advance(left_two, left, current, right):
        return [
            (c * (1.0 - TIME_STEP) + FORCING * TIME_STEP * TIME_STEP) + (d - a) * b
            for a, b, c, d in zip(left_two, left, current, right, strict=True)
        ]

    def store(cell, values):
        for half in range(halves):
            begin = cell * tiles + half * ROWS
            state_ref[begin : begin + ROWS, :] = values[half]

    def substep(_, carry):
        before_two = previous_run(group(LANES - 2))
        before = previous_run(group(LANES - 1))
        first = [group(cell) for cell in range(3)]
        beyond = next_run(first[0])
        window = list(first)
        for cell in range(2, LANES - 1):
            right = group(cell + 1)
            store(cell, advance(*window, right))
            window = window[1:] + [right]
        store(LANES - 1, advance(*window, beyond))
        store(0, advance(before_two, before, first[0], first[1]))
        store(1, advance(before, first[0], first[1], first[2]))
        return carry

    lax.fori_loop(0, PREDICT_SUBTICKS, substep, 0)

    for cell in range(LANES):
        for half in range(halves):
            begin = cell * cell_pitch + half * ROWS
            tile_ref[begin : begin + ROWS, :] = group(cell)[half]
    for tile in range(tiles):
        state_ref[tile * LANES : (tile + 1) * LANES, :] = tile_ref[pl.ds(tile, LANES, stride=cell_pitch), :].T * (1.0 / TIME_STEP)

    def gather(block, carry):
        base = block * LANES
        picked = [jnp.zeros((ROWS, LANES), jnp.float32) for _ in range(4)]
        for number in range(LANES):
            place = places_ref[base + number]
            begin = pl.multiple_of((place // (LANES * parts)) * ROWS, ROWS)
            turned = pltpu.roll(state_ref[pl.ds(begin, ROWS), :], (number - place) & (LANES - 1), axis=1)
            picked[number % 4] = jnp.where(lane == number, turned, picked[number % 4])
        both = picked[0]
        for number in range(1, 4):
            both = jnp.where(lane % 4 == number, picked[number], both)
        part_of = (runs_ref[pl.ds(block, 1), :] // LANES) % parts
        chosen = both
        for part in range(1, parts):
            chosen = jnp.where(part_of == part, pltpu.roll(both, ROWS - part * members, axis=0), chosen)
        for destination in range(devices):
            readings_ref[destination, pl.ds(block * members, members), :] = chosen[:members]
        return carry

    lax.fori_loop(0, runs_ref.shape[0], gather, 0)


def dot(a, b, contract, precision=HIGH):
    return lax.dot_general(a, b, (contract, ((), ())), precision=precision, preferred_element_type=jnp.float32)


def split_three(value):
    high = value.astype(jnp.bfloat16)
    rest = value - high.astype(jnp.float32)
    middle = rest.astype(jnp.bfloat16)
    return high, middle, (rest - middle.astype(jnp.float32)).astype(jnp.bfloat16)


def invert_all(matrix_ref):
    regions, size, _ = matrix_ref.shape
    lane = lanes_iota()
    row = rows_iota()

    def panel(number, carry):
        base = number * ROWS
        start = pl.multiple_of(base, ROWS)
        offset = lane - base
        inside = (offset >= 0) & (offset < ROWS)
        unit = jnp.where(offset == row, 1.0, 0.0)
        blocks = [matrix_ref[region, pl.ds(start, ROWS), :] for region in range(regions)]
        columns = []
        for k in range(ROWS):
            index = jnp.full((ROWS, LANES), base + k, jnp.int32)
            columns.append([jnp.take_along_axis(block, index, axis=1) for block in blocks])
        lefts = []
        for block in blocks:
            signed = jnp.where(inside, 0.0, jnp.where(offset < 0, block, -block))
            high, middle, low = split_three(signed)
            lefts.append(jnp.concatenate([high, high, middle, high, low, middle], axis=0))
        blocks = [jnp.where(inside, unit, block) for block in blocks]
        for j in range(ROWS):
            here = row == j
            for region in range(regions):
                pivot = columns[j][region]
                inverse = 1.0 / pivot[j : j + 1, :]
                scaled = blocks[region][j : j + 1, :] * inverse
                blocks[region] = jnp.where(here, scaled, blocks[region] - pivot * scaled)
                for k in range(j + 1, ROWS):
                    scaled = columns[k][region][j : j + 1, :] * inverse
                    columns[k][region] = jnp.where(here, scaled, columns[k][region] - pivot * scaled)
        for region in range(regions):
            high, middle, low = split_three(blocks[region])
            right = jnp.concatenate([high, middle, high, low, high, middle], axis=0)
            update = dot(lefts[region], right, ((0,), (0,)), lax.Precision.DEFAULT)
            for i in range(size // ROWS):
                rows = slice(i * ROWS, (i + 1) * ROWS)
                matrix_ref[region, rows, :] = jnp.where(inside, 0.0, matrix_ref[region, rows, :]) + update[rows]
            matrix_ref[region, pl.ds(start, ROWS), :] = blocks[region]
        return carry

    lax.fori_loop(0, size // ROWS, panel, 0)


def solve_kernel(
    zone_ref, neighbours_ref, table_ref, readings_ref, noise_ref, transform_ref, stack_ref, pieces_ref, matrix_ref, *, cells, zone_cells
):
    devices, _, _ = readings_ref.shape
    regions, total, _ = transform_ref.shape
    members = total // devices
    observations = table_ref.shape[1]
    extra = stack_ref.shape[0] - 2 * total
    for block in range(observations // LANES):
        lanes = slice(block * LANES, (block + 1) * LANES)
        values = table_ref[0:1, lanes]
        spread = jnp.sqrt(table_ref[1:2, lanes])
        for source in range(devices):
            equivalents = readings_ref[source, block * members : (block + 1) * members, :]
            noise = noise_ref[source, block * members : (block + 1) * members, :]
            stack_ref[source * members : (source + 1) * members, lanes] = equivalents
            stack_ref[total + source * members : total + (source + 1) * members, lanes] = values + spread * noise - equivalents
    stack_ref[2 * total : 2 * total + ROWS, :] = table_ref[...]
    stack_ref[2 * total + ROWS :, :] = jnp.zeros((extra - ROWS, observations), jnp.float32)
    height = stack_ref.shape[0]
    rest = stack_ref[...]
    for piece in range(3):
        rounded = rest.astype(jnp.bfloat16)
        pieces_ref[piece * height : (piece + 1) * height, :] = rounded
        rest = rest - rounded.astype(jnp.float32)

    centre0 = zone_ref[0] * zone_cells + zone_cells // 2
    size = neighbours_ref.shape[1]
    diagonal = lax.broadcasted_iota(jnp.int32, (size, size), 0) == lax.broadcasted_iota(jnp.int32, (size, size), 1)
    ids = lax.broadcasted_iota(jnp.int32, (observations, size), 0)
    anomalies, innovations = [], []
    for region in range(regions):
        pick = jnp.where(ids == neighbours_ref[region : region + 1, :], 1.0, 0.0).astype(jnp.bfloat16)
        picked = dot(pieces_ref[...], pick, ((1,), (0,)), lax.Precision.DEFAULT)
        picked = picked[:height] + picked[height : 2 * height] + picked[2 * height :]
        equivalents = picked[:total]
        innovations.append(picked[total : 2 * total])
        variance = picked[2 * total + 1 : 2 * total + 2]
        place = picked[2 * total + 2 : 2 * total + 3]
        centre = (centre0 + region * zone_cells).astype(jnp.float32)
        gap = jnp.abs(place - centre)
        scaled = jnp.minimum(gap, cells - gap) / float(LSCALE)
        errors = variance * (1.0 + scaled * scaled)
        anomaly = equivalents - jnp.sum(equivalents, axis=0, keepdims=True) * (1.0 / total)
        anomalies.append(anomaly)
        covariance = dot(anomaly, anomaly, ((0,), (0,))) * (1.0 / (total - 1))
        matrix_ref[region, :, :] = jnp.where(diagonal, covariance + errors, covariance)
    invert_all(matrix_ref)
    for region in range(regions):
        weights = dot(innovations[region], matrix_ref[region], ((1,), (0,)))
        transform_ref[region, :, :] = dot(weights, anomalies[region], ((1,), (1,))) * (1.0 / (total - 1))


def apply_kernel(counts_ref, transform_ref, cells_ref, owned_ref, block_ref, result_ref):
    sources, height, _ = cells_ref.shape
    regions, total, _ = transform_ref.shape
    members = total // sources
    tiles = height // members
    wide = tiles // regions
    for tile in range(tiles):
        region, place = tile // wide, tile % wide
        for source in range(sources):
            block_ref[region, source * members : (source + 1) * members, place * LANES : (place + 1) * LANES] = cells_ref[
                source, tile * members : (tile + 1) * members, :
            ]
    for region in range(regions):
        block = block_ref[region]
        anomalies = block - jnp.sum(block, axis=0, keepdims=True) * (1.0 / total)
        analysed = block + dot(transform_ref[region], anomalies, ((1,), (0,)))
        for place in range(wide):
            result_ref[region * wide + place, :total, :] = analysed[:, place * LANES : (place + 1) * LANES]
    for tile in range(tiles):
        result_ref[tile, total:, :] = jnp.zeros((ROWS, LANES), jnp.float32)

    def window(destination, offset):
        for tile in range(tiles):
            owned_ref[destination, tile * ROWS : (tile + 1) * ROWS, :] = result_ref[tile, pl.ds(offset, CAP), :]
        return offset + counts_ref[destination]

    lax.fori_loop(0, sources, window, jnp.int32(0))


def advance_kernel(count_ref, rows_ref, out_ref):
    tiles = rows_ref.shape[0] // ROWS
    here = out_ref.shape[1] // LANES
    lane = lanes_iota()
    occupied = rows_iota() < count_ref[0]
    start = pl.program_id(0) * here

    def load(number):
        return rows_ref[pl.ds(pl.multiple_of(number * ROWS, ROWS), ROWS), :]

    before = load(lax.rem(start + tiles - 1, tiles))
    before_one = pltpu.roll(before, 1, axis=1)
    before_two = pltpu.roll(before, 2, axis=1)
    current = load(start)
    current_up = pltpu.roll(current, LANES - 1, axis=1)
    for tile in range(here):
        after = load(start + tile + 1) if tile + 1 < here else load(lax.rem(start + here, tiles))
        after_up = pltpu.roll(after, LANES - 1, axis=1)
        one = pltpu.roll(current, 1, axis=1)
        two = pltpu.roll(current, 2, axis=1)
        left = jnp.where(lane == 0, before_one, one)
        left_two = jnp.where(lane < 2, before_two, two)
        right = jnp.where(lane == LANES - 1, after_up, current_up)
        stepped = current + TIME_STEP * ((right - left_two) * left - current + FORCING)
        out_ref[:, tile * LANES : (tile + 1) * LANES] = jnp.where(occupied, stepped, 0.0)
        before_one, before_two = one, two
        current, current_up = after, after_up


def whole(space=pltpu.VMEM):
    return pl.BlockSpec(memory_space=space)


def per_device(prior_sample_matrix, obs_values, obs_var, measured_indexes, neighbours, perturbation, counts):
    devices = lax.axis_size(AXES)
    device_index = lax.axis_index(AXES)
    members, cells = prior_sample_matrix.shape
    total = members * devices
    observations = obs_values.shape[0]
    zones, local = neighbours.shape
    regions = zones // devices
    zone_cells = cells // zones
    share = cells // devices
    blocks = observations // LANES

    runs = prior_sample_matrix.reshape(members, cells // LANES, LANES).transpose(1, 0, 2).reshape(-1, LANES)
    height = runs.shape[0]
    tiles = height // LANES
    state, readings = pl.pallas_call(
        functools.partial(forecast_kernel, devices=devices, members=members),
        out_shape=(
            jax.ShapeDtypeStruct((height, LANES), jnp.float32),
            jax.ShapeDtypeStruct((devices, blocks * members, LANES), jnp.float32),
        ),
        in_specs=[whole(pltpu.SMEM), whole(), whole()],
        out_specs=(whole(), whole()),
        scratch_shapes=[pltpu.VMEM((max(tiles * (LANES + ROWS), LANES * (tiles + ROWS)), LANES), jnp.float32)],
        name="forecast",
    )(measured_indexes, measured_indexes.reshape(blocks, LANES), runs)

    noise = perturbation.reshape(members, blocks, LANES).transpose(1, 0, 2).reshape(1, blocks * members, LANES)
    exchange = functools.partial(lax.all_to_all, axis_name=AXES, split_axis=0, concat_axis=0, tiled=True)
    noise = exchange(jnp.broadcast_to(noise, (devices, blocks * members, LANES)))
    readings = exchange(readings)
    own_cells = exchange(state.reshape(devices, height // devices, LANES))

    zone = device_index * regions
    table = jnp.stack([obs_values, obs_var, measured_indexes.astype(jnp.float32)])
    table = jnp.concatenate([table, jnp.zeros((ROWS - 3, observations), jnp.float32)])
    height = 2 * total + 2 * ROWS
    transform = pl.pallas_call(
        functools.partial(solve_kernel, cells=float(cells), zone_cells=zone_cells),
        out_shape=jax.ShapeDtypeStruct((regions, total, total), jnp.float32),
        in_specs=[whole(pltpu.SMEM), whole(), whole(), whole(), whole()],
        out_specs=whole(),
        scratch_shapes=[
            pltpu.VMEM((height, observations), jnp.float32),
            pltpu.VMEM((3 * height, observations), jnp.bfloat16),
            pltpu.VMEM((regions, local, local), jnp.float32),
        ],
        name="solve",
    )(zone.reshape(1), lax.dynamic_slice_in_dim(neighbours, zone, regions, 0), table, readings, noise)

    tiles = share // LANES
    outgoing = pl.pallas_call(
        apply_kernel,
        out_shape=jax.ShapeDtypeStruct((devices, tiles * CAP, LANES), jnp.float32),
        in_specs=[whole(pltpu.SMEM), whole(), whole()],
        out_specs=whole(),
        scratch_shapes=[
            pltpu.VMEM((regions, total, zone_cells), jnp.float32),
            pltpu.VMEM((tiles, total + ROWS, LANES), jnp.float32),
        ],
        name="analyse",
    )(counts, transform, own_cells)
    owned = exchange(outgoing).reshape(devices * tiles * CAP, LANES)

    chunks = 8
    return pl.pallas_call(
        advance_kernel,
        grid=(chunks,),
        out_shape=jax.ShapeDtypeStruct((CAP, cells), jnp.float32),
        in_specs=[whole(pltpu.SMEM), whole()],
        out_specs=pl.BlockSpec((CAP, cells // chunks), lambda i: (0, i)),
        name="advance",
    )(lax.dynamic_slice_in_dim(counts, device_index, 1, 0), owned)


def solution(mesh):
    rows = P(AXES, None)
    return jax.shard_map(
        per_device, mesh=mesh, in_specs=(rows, P(), P(), P(), P(), rows, P()), out_specs=rows, check_vma=False
    )
```

```python
import functools

import jax
import jax.numpy as jnp
from jax import lax
from jax.experimental import pallas as pl
from jax.experimental.pallas import tpu as pltpu
from jax.sharding import PartitionSpec as P

PREDICT_SUBTICKS = 24
CAP = 8
LSCALE = 2048
FORCING = 8.0
TIME_STEP = 0.01
HIGH = lax.Precision.HIGHEST
AXES = ("member", "region")
LANES = 128
ROWS = 8


def lanes_iota():
    return lax.broadcasted_iota(jnp.int32, (ROWS, LANES), 1)


def rows_iota():
    return lax.broadcasted_iota(jnp.int32, (ROWS, LANES), 0)


def forecast_kernel(places_ref, x_ref, *refs, devices, members):
    *chunk_refs, readings_ref, state_ref, tile_ref, table_ref, scalar_ref, table_sem = refs
    height = x_ref.shape[0]
    blocks = places_ref.shape[0]
    tiles = height // LANES
    halves = tiles // ROWS
    tile_pitch = LANES + ROWS
    cell_pitch = tiles + ROWS
    parts = ROWS // members
    lane = lanes_iota()
    row = rows_iota()

    def group(cell):
        return [state_ref[cell * tiles + half * ROWS : cell * tiles + (half + 1) * ROWS, :] for half in range(halves)]

    for tile in range(tiles):
        tile_ref[tile * tile_pitch : tile * tile_pitch + LANES, :] = (x_ref[tile * LANES : (tile + 1) * LANES, :] * TIME_STEP).T
    for cell in range(LANES):
        for half in range(halves):
            begin = cell * tiles + half * ROWS
            state_ref[begin : begin + ROWS, :] = tile_ref[pl.ds(half * ROWS * tile_pitch + cell, ROWS, stride=tile_pitch), :]

    places = places_ref[...]
    column = lax.broadcasted_iota(jnp.int32, places.shape, 1)
    table_ref[:blocks, :] = (places // (LANES * parts)) * ROWS
    table_ref[blocks:, :] = (column - places) & (LANES - 1)
    table_copy = pltpu.make_async_copy(table_ref, scalar_ref, table_sem)
    table_copy.start()

    def next_run(values):
        turned = [pltpu.roll(value, LANES - members, axis=1) for value in values]
        down = [pltpu.roll(value, ROWS - 1, axis=0) for value in turned]
        carried = [jnp.where(row == ROWS - 1, down[(half + 1) % halves], down[half]) for half in range(halves)]
        return [jnp.where(lane >= LANES - members, carry, value) for carry, value in zip(carried, turned, strict=True)]

    def previous_run(values):
        turned = [pltpu.roll(value, members, axis=1) for value in values]
        up = [pltpu.roll(value, 1, axis=0) for value in turned]
        carried = [jnp.where(row == 0, up[half - 1], up[half]) for half in range(halves)]
        return [jnp.where(lane < members, carry, value) for carry, value in zip(carried, turned, strict=True)]

    def advance(left_two, left, current, right):
        return [
            (c * (1.0 - TIME_STEP) + FORCING * TIME_STEP * TIME_STEP) + (d - a) * b
            for a, b, c, d in zip(left_two, left, current, right, strict=True)
        ]

    def store(cell, values):
        for half in range(halves):
            begin = cell * tiles + half * ROWS
            state_ref[begin : begin + ROWS, :] = values[half]

    def substep(_, carry):
        before_two = previous_run(group(LANES - 2))
        before = previous_run(group(LANES - 1))
        first = [group(cell) for cell in range(3)]
        beyond = next_run(first[0])
        window = list(first)
        for cell in range(2, LANES - 1):
            right = group(cell + 1)
            store(cell, advance(*window, right))
            window = window[1:] + [right]
        store(LANES - 1, advance(*window, beyond))
        store(0, advance(before_two, before, first[0], first[1]))
        store(1, advance(before, first[0], first[1], first[2]))
        return carry

    lax.fori_loop(0, PREDICT_SUBTICKS, substep, 0)

    for cell in range(LANES):
        for half in range(halves):
            begin = cell * cell_pitch + half * ROWS
            tile_ref[begin : begin + ROWS, :] = group(cell)[half]
    for tile in range(tiles):
        state_ref[tile * LANES : (tile + 1) * LANES, :] = tile_ref[pl.ds(tile, LANES, stride=cell_pitch), :].T * (1.0 / TIME_STEP)
    share = height // devices
    part_rows = share // len(chunk_refs)
    for destination in range(devices):
        for number, chunk_ref in enumerate(chunk_refs):
            begin = destination * share + number * part_rows
            chunk_ref[destination, :, :] = state_ref[begin : begin + part_rows, :]
    table_copy.wait()

    def gather(block, carry):
        picked = [jnp.zeros((ROWS, LANES), jnp.float32) for _ in range(4)]
        for number in range(LANES):
            begin = pl.multiple_of(scalar_ref[block, number], ROWS)
            turned = pltpu.roll(state_ref[pl.ds(begin, ROWS), :], scalar_ref[blocks + block, number], axis=1)
            picked[number % 4] = jnp.where(lane == number, turned, picked[number % 4])
        both = picked[0]
        for number in range(1, 4):
            both = jnp.where(lane % 4 == number, picked[number], both)
        part_of = (places_ref[pl.ds(block, 1), :] // LANES) % parts
        chosen = both
        for part in range(1, parts):
            chosen = jnp.where(part_of == part, pltpu.roll(both, ROWS - part * members, axis=0), chosen)
        for destination in range(devices):
            readings_ref[destination, pl.ds(block * members, members), :] = chosen[:members]
        return carry

    lax.fori_loop(0, blocks, gather, 0)


def dot(a, b, contract, precision=HIGH):
    return lax.dot_general(a, b, (contract, ((), ())), precision=precision, preferred_element_type=jnp.float32)


def split_three(value):
    high = value.astype(jnp.bfloat16)
    rest = value - high.astype(jnp.float32)
    middle = rest.astype(jnp.bfloat16)
    return high, middle, (rest - middle.astype(jnp.float32)).astype(jnp.bfloat16)


def invert_all(matrix_ref):
    regions, size, _ = matrix_ref.shape
    lane = lanes_iota()
    row = rows_iota()

    def panel(number, carry):
        base = number * ROWS
        start = pl.multiple_of(base, ROWS)
        offset = lane - base
        inside = (offset >= 0) & (offset < ROWS)
        unit = jnp.where(offset == row, 1.0, 0.0)
        blocks = [matrix_ref[region, pl.ds(start, ROWS), :] for region in range(regions)]
        columns = []
        for k in range(ROWS):
            index = jnp.full((ROWS, LANES), base + k, jnp.int32)
            columns.append([jnp.take_along_axis(block, index, axis=1) for block in blocks])
        lefts = []
        for block in blocks:
            signed = jnp.where(inside, 0.0, jnp.where(offset < 0, block, -block))
            high, middle, low = split_three(signed)
            lefts.append(jnp.concatenate([high, high, middle, high, low, middle], axis=0))
        blocks = [jnp.where(inside, unit, block) for block in blocks]
        for j in range(ROWS):
            here = row == j
            for region in range(regions):
                pivot = columns[j][region]
                inverse = 1.0 / pivot[j : j + 1, :]
                scaled = blocks[region][j : j + 1, :] * inverse
                blocks[region] = jnp.where(here, scaled, blocks[region] - pivot * scaled)
                for k in range(j + 1, ROWS):
                    scaled = columns[k][region][j : j + 1, :] * inverse
                    columns[k][region] = jnp.where(here, scaled, columns[k][region] - pivot * scaled)
        for region in range(regions):
            high, middle, low = split_three(blocks[region])
            right = jnp.concatenate([high, middle, high, low, high, middle], axis=0)
            update = dot(lefts[region], right, ((0,), (0,)), lax.Precision.DEFAULT)
            for i in range(size // ROWS):
                rows = slice(i * ROWS, (i + 1) * ROWS)
                matrix_ref[region, rows, :] = jnp.where(inside, 0.0, matrix_ref[region, rows, :]) + update[rows]
            matrix_ref[region, pl.ds(start, ROWS), :] = blocks[region]
        return carry

    lax.fori_loop(0, size // ROWS, panel, 0)


def store_pieces(pieces_ref, value):
    height = value.shape[0]
    for number, piece in enumerate(split_three(value)):
        pieces_ref[number * height : (number + 1) * height, :] = piece


def select(pieces_ref, pick):
    height = pieces_ref.shape[0] // 3
    picked = dot(pieces_ref[...], pick, ((1,), (0,)), lax.Precision.DEFAULT)
    return picked[:height] + picked[height : 2 * height] + picked[2 * height :]


def spread_rows(stack_ref, source_ref, offset, members, convert):
    sources, height, _ = source_ref.shape
    for block in range(height // members):
        lanes = slice(block * LANES, (block + 1) * LANES)
        for source in range(sources):
            begin = offset + source * members
            stack_ref[begin : begin + members, lanes] = convert(lanes, source_ref[source, block * members : (block + 1) * members, :])


def prepare_kernel(zone_ref, neighbours_ref, table_ref, noise_ref, pick_ref, errors_ref, target_ref, stack_ref, pieces_ref, *, cells, zone_cells):
    regions, total, _ = target_ref.shape
    members = total // noise_ref.shape[0]
    observations = table_ref.shape[1]
    size = neighbours_ref.shape[1]
    spread_rows(
        stack_ref,
        noise_ref,
        0,
        members,
        lambda lanes, noise: table_ref[0:1, lanes] + jnp.sqrt(table_ref[1:2, lanes]) * noise,
    )
    stack_ref[total : total + ROWS, :] = table_ref[...]
    stack_ref[total + ROWS :, :] = jnp.zeros((ROWS, observations), jnp.float32)
    store_pieces(pieces_ref, stack_ref[...])
    ids = lax.broadcasted_iota(jnp.int32, (observations, size), 0)
    for region in range(regions):
        pick = jnp.where(ids == neighbours_ref[region : region + 1, :], 1.0, 0.0).astype(jnp.bfloat16)
        pick_ref[region, :, :] = pick
        picked = select(pieces_ref, pick)
        target_ref[region, :, :] = picked[:total]
        variance = picked[total + 1 : total + 2]
        place = picked[total + 2 : total + 3]
        centre = ((zone_ref[0] + region) * zone_cells + zone_cells // 2).astype(jnp.float32)
        gap = jnp.abs(place - centre)
        scaled = jnp.minimum(gap, cells - gap) / float(LSCALE)
        errors_ref[region : region + 1, :] = variance * (1.0 + scaled * scaled)


def solve_kernel(pick_ref, errors_ref, target_ref, readings_ref, transform_ref, stack_ref, pieces_ref, matrix_ref):
    regions, total, _ = transform_ref.shape
    members = total // readings_ref.shape[0]
    size = pick_ref.shape[2]
    spread_rows(stack_ref, readings_ref, 0, members, lambda lanes, value: value)
    store_pieces(pieces_ref, stack_ref[...])
    diagonal = lax.broadcasted_iota(jnp.int32, (size, size), 0) == lax.broadcasted_iota(jnp.int32, (size, size), 1)
    anomalies, innovations = [], []
    for region in range(regions):
        equivalents = select(pieces_ref, pick_ref[region])
        innovations.append(target_ref[region] - equivalents)
        anomaly = equivalents - jnp.sum(equivalents, axis=0, keepdims=True) * (1.0 / total)
        anomalies.append(anomaly)
        covariance = dot(anomaly, anomaly, ((0,), (0,))) * (1.0 / (total - 1))
        matrix_ref[region, :, :] = jnp.where(diagonal, covariance + errors_ref[region : region + 1, :], covariance)
    invert_all(matrix_ref)
    for region in range(regions):
        weights = dot(innovations[region], matrix_ref[region], ((1,), (0,)))
        transform_ref[region, :, :] = dot(weights, anomalies[region], ((1,), (1,))) * (1.0 / (total - 1))


def apply_kernel(counts_ref, transform_ref, cells_ref, owned_ref, block_ref, result_ref, *, first, wide):
    sources, height, _ = cells_ref.shape
    _, total, _ = transform_ref.shape
    members = total // sources
    tiles = height // members
    for tile in range(tiles):
        lanes = slice(tile * LANES, (tile + 1) * LANES)
        for source in range(sources):
            block_ref[source * members : (source + 1) * members, lanes] = cells_ref[source, tile * members : (tile + 1) * members, :]
    tile = 0
    while tile < tiles:
        region = (first + tile) // wide
        until = min(tiles, (region + 1) * wide - first)
        block = block_ref[:, tile * LANES : until * LANES]
        anomalies = block - jnp.sum(block, axis=0, keepdims=True) * (1.0 / total)
        analysed = block + dot(transform_ref[region], anomalies, ((1,), (0,)))
        for number in range(tile, until):
            result_ref[number, :total, :] = analysed[:, (number - tile) * LANES : (number - tile + 1) * LANES]
        tile = until
    for tile in range(tiles):
        result_ref[tile, total:, :] = jnp.zeros((ROWS, LANES), jnp.float32)

    def window(destination, offset):
        for tile in range(tiles):
            owned_ref[destination, tile * ROWS : (tile + 1) * ROWS, :] = result_ref[tile, pl.ds(offset, CAP), :]
        return offset + counts_ref[destination]

    lax.fori_loop(0, sources, window, jnp.int32(0))


def advance_kernel(count_ref, *refs):
    *chunk_refs, out_ref = refs
    sources, height, _ = chunk_refs[0].shape
    share = height // ROWS
    tiles = share * len(chunk_refs)
    here = out_ref.shape[1] // LANES // tiles
    lane = lanes_iota()
    occupied = rows_iota() < count_ref[0]
    start = pl.program_id(0) * here

    def load(source, tile):
        return chunk_refs[tile // share][source, (tile % share) * ROWS : (tile % share + 1) * ROWS, :]

    before = load(lax.rem(start + sources - 1, sources), tiles - 1)
    before_one = pltpu.roll(before, 1, axis=1)
    before_two = pltpu.roll(before, 2, axis=1)
    current = load(start, 0)
    current_up = pltpu.roll(current, LANES - 1, axis=1)
    for number in range(here * tiles):
        source, tile = divmod(number + 1, tiles)
        after = load(start + source if source < here else lax.rem(start + here, sources), tile)
        after_up = pltpu.roll(after, LANES - 1, axis=1)
        one = pltpu.roll(current, 1, axis=1)
        two = pltpu.roll(current, 2, axis=1)
        left = jnp.where(lane == 0, before_one, one)
        left_two = jnp.where(lane < 2, before_two, two)
        right = jnp.where(lane == LANES - 1, after_up, current_up)
        stepped = current + TIME_STEP * ((right - left_two) * left - current + FORCING)
        out_ref[:, number * LANES : (number + 1) * LANES] = jnp.where(occupied, stepped, 0.0)
        before_one, before_two = one, two
        current, current_up = after, after_up


def whole(space=pltpu.VMEM):
    return pl.BlockSpec(memory_space=space)


CHUNKS = 1


def in_vmem(value):
    return pltpu.with_memory_space_constraint(value, pltpu.VMEM)


def per_device(prior_sample_matrix, obs_values, obs_var, measured_indexes, neighbours, perturbation, counts):
    devices = lax.axis_size(AXES)
    device_index = lax.axis_index(AXES)
    members, cells = prior_sample_matrix.shape
    total = members * devices
    observations = obs_values.shape[0]
    zones, local = neighbours.shape
    regions = zones // devices
    zone_cells = cells // zones
    blocks = observations // LANES
    share_tiles = cells // devices // LANES
    chunk_tiles = share_tiles // CHUNKS
    exchange = functools.partial(lax.all_to_all, axis_name=AXES, split_axis=0, concat_axis=0, tiled=True)

    def by_block(value):
        return value.reshape(devices, members, blocks, LANES).transpose(0, 2, 1, 3).reshape(devices, blocks * members, LANES)

    noise = by_block(exchange(jnp.broadcast_to(perturbation[None], (devices, members, observations))))

    runs = prior_sample_matrix.reshape(members, cells // LANES, LANES).transpose(1, 0, 2).reshape(-1, LANES)
    height = runs.shape[0]
    tiles = height // LANES
    chunk_shape = jax.ShapeDtypeStruct((devices, chunk_tiles * members, LANES), jnp.float32)
    *states, readings = pl.pallas_call(
        functools.partial(forecast_kernel, devices=devices, members=members),
        out_shape=(chunk_shape,) * CHUNKS + (jax.ShapeDtypeStruct((devices, blocks * members, LANES), jnp.float32),),
        in_specs=[whole(), whole()],
        out_specs=(whole(),) * (CHUNKS + 1),
        scratch_shapes=[
            pltpu.VMEM((height, LANES), jnp.float32),
            pltpu.VMEM((max(tiles * (LANES + ROWS), LANES * (tiles + ROWS)), LANES), jnp.float32),
            pltpu.VMEM((2 * blocks, LANES), jnp.int32),
            pltpu.SMEM((2 * blocks, LANES), jnp.int32),
            pltpu.SemaphoreType.DMA,
        ],
        name="forecast",
    )(measured_indexes.reshape(blocks, LANES), runs)

    readings = exchange(readings)
    own_cells = [exchange(state) for state in states]

    zone = device_index * regions
    table = jnp.stack([obs_values, obs_var, measured_indexes.astype(jnp.float32)])
    table = jnp.concatenate([table, jnp.zeros((ROWS - 3, observations), jnp.float32)])
    pick, errors, target = pl.pallas_call(
        functools.partial(prepare_kernel, cells=float(cells), zone_cells=zone_cells),
        out_shape=(
            jax.ShapeDtypeStruct((regions, observations, local), jnp.bfloat16),
            jax.ShapeDtypeStruct((regions, local), jnp.float32),
            jax.ShapeDtypeStruct((regions, total, local), jnp.float32),
        ),
        in_specs=[whole(pltpu.SMEM), whole(), whole(), whole()],
        out_specs=(whole(),) * 3,
        scratch_shapes=[
            pltpu.VMEM((total + 2 * ROWS, observations), jnp.float32),
            pltpu.VMEM((3 * (total + 2 * ROWS), observations), jnp.bfloat16),
        ],
        name="prepare",
    )(zone.reshape(1), lax.dynamic_slice_in_dim(neighbours, zone, regions, 0), table, in_vmem(noise))
    transform = pl.pallas_call(
        solve_kernel,
        out_shape=jax.ShapeDtypeStruct((regions, total, total), jnp.float32),
        in_specs=[whole()] * 4,
        out_specs=whole(),
        scratch_shapes=[
            pltpu.VMEM((total, observations), jnp.float32),
            pltpu.VMEM((3 * total, observations), jnp.bfloat16),
            pltpu.VMEM((regions, local, local), jnp.float32),
        ],
        name="solve",
    )(pick, errors, target, in_vmem(readings))
    transform = in_vmem(transform)

    owned = []
    for number in range(CHUNKS):
        outgoing = pl.pallas_call(
            functools.partial(apply_kernel, first=number * chunk_tiles, wide=zone_cells // LANES),
            out_shape=jax.ShapeDtypeStruct((devices, chunk_tiles * CAP, LANES), jnp.float32),
            in_specs=[whole(pltpu.SMEM), whole(), whole()],
            out_specs=whole(),
            scratch_shapes=[
                pltpu.VMEM((total, chunk_tiles * LANES), jnp.float32),
                pltpu.VMEM((chunk_tiles, total + ROWS, LANES), jnp.float32),
            ],
            name=f"analyse{number}",
        )(counts, transform, in_vmem(own_cells[number]))
        owned.append(in_vmem(exchange(outgoing)))

    steps = 8
    return pl.pallas_call(
        advance_kernel,
        grid=(steps,),
        out_shape=jax.ShapeDtypeStruct((CAP, cells), jnp.float32),
        in_specs=[whole(pltpu.SMEM)] + [whole()] * CHUNKS,
        out_specs=pl.BlockSpec((CAP, cells // steps), lambda i: (0, i)),
        name="advance",
    )(lax.dynamic_slice_in_dim(counts, device_index, 1, 0), *owned)


def solution(mesh):
    rows = P(AXES, None)
    return jax.shard_map(
        per_device, mesh=mesh, in_specs=(rows, P(), P(), P(), P(), rows, P()), out_specs=rows, check_vma=False
    )
```

```python
import functools

import jax
import jax.numpy as jnp
from jax import lax
from jax.experimental import pallas as pl
from jax.experimental.pallas import tpu as pltpu
from jax.sharding import PartitionSpec as P

PREDICT_SUBTICKS = 24
CAP = 8
LSCALE = 2048
FORCING = 8.0
TIME_STEP = 0.01
HIGH = lax.Precision.HIGHEST
AXES = ("member", "region")
LANES = 128
ROWS = 8


def lanes_iota():
    return lax.broadcasted_iota(jnp.int32, (ROWS, LANES), 1)


def rows_iota():
    return lax.broadcasted_iota(jnp.int32, (ROWS, LANES), 0)


def forecast_kernel(places_ref, noise_ref, x_ref, state_ref, mine_ref, tile_ref, table_ref, scalar_ref, table_sem, *, members):
    height = x_ref.shape[0]
    blocks = places_ref.shape[0]
    tiles = height // LANES
    halves = tiles // ROWS
    tile_pitch = LANES + ROWS
    cell_pitch = tiles + ROWS
    parts = ROWS // members
    lane = lanes_iota()
    row = rows_iota()

    def group(cell):
        return [state_ref[cell * tiles + half * ROWS : cell * tiles + (half + 1) * ROWS, :] for half in range(halves)]

    for tile in range(tiles):
        tile_ref[tile * tile_pitch : tile * tile_pitch + LANES, :] = (x_ref[tile * LANES : (tile + 1) * LANES, :] * TIME_STEP).T
    for cell in range(LANES):
        for half in range(halves):
            begin = cell * tiles + half * ROWS
            state_ref[begin : begin + ROWS, :] = tile_ref[pl.ds(half * ROWS * tile_pitch + cell, ROWS, stride=tile_pitch), :]

    places = places_ref[...]
    column = lax.broadcasted_iota(jnp.int32, places.shape, 1)
    table_ref[:blocks, :] = (places // (LANES * parts)) * ROWS
    table_ref[blocks:, :] = (column - places) & (LANES - 1)
    table_copy = pltpu.make_async_copy(table_ref, scalar_ref, table_sem)
    table_copy.start()

    def next_run(values):
        turned = [pltpu.roll(value, LANES - members, axis=1) for value in values]
        down = [pltpu.roll(value, ROWS - 1, axis=0) for value in turned]
        carried = [jnp.where(row == ROWS - 1, down[(half + 1) % halves], down[half]) for half in range(halves)]
        return [jnp.where(lane >= LANES - members, carry, value) for carry, value in zip(carried, turned, strict=True)]

    def previous_run(values):
        turned = [pltpu.roll(value, members, axis=1) for value in values]
        up = [pltpu.roll(value, 1, axis=0) for value in turned]
        carried = [jnp.where(row == 0, up[half - 1], up[half]) for half in range(halves)]
        return [jnp.where(lane < members, carry, value) for carry, value in zip(carried, turned, strict=True)]

    def advance(left_two, left, current, right):
        return [
            (c * (1.0 - TIME_STEP) + FORCING * TIME_STEP * TIME_STEP) + (d - a) * b
            for a, b, c, d in zip(left_two, left, current, right, strict=True)
        ]

    def store(cell, values):
        for half in range(halves):
            begin = cell * tiles + half * ROWS
            state_ref[begin : begin + ROWS, :] = values[half]

    def substep(_, carry):
        before_two = previous_run(group(LANES - 2))
        before = previous_run(group(LANES - 1))
        first = [group(cell) for cell in range(3)]
        beyond = next_run(first[0])
        window = list(first)
        for cell in range(2, LANES - 1):
            right = group(cell + 1)
            store(cell, advance(*window, right))
            window = window[1:] + [right]
        store(LANES - 1, advance(*window, beyond))
        store(0, advance(before_two, before, first[0], first[1]))
        store(1, advance(before, first[0], first[1], first[2]))
        return carry

    lax.fori_loop(0, PREDICT_SUBTICKS, substep, 0)

    for cell in range(LANES):
        for half in range(halves):
            begin = cell * cell_pitch + half * ROWS
            tile_ref[begin : begin + ROWS, :] = group(cell)[half]
    for tile in range(tiles):
        state_ref[tile * LANES : (tile + 1) * LANES, :] = tile_ref[pl.ds(tile, LANES, stride=cell_pitch), :].T * (1.0 / TIME_STEP)
    table_copy.wait()

    def gather(block, carry):
        picked = [jnp.zeros((ROWS, LANES), jnp.float32) for _ in range(4)]
        for number in range(LANES):
            begin = pl.multiple_of(scalar_ref[block, number], ROWS)
            turned = pltpu.roll(state_ref[pl.ds(begin, ROWS), :], scalar_ref[blocks + block, number], axis=1)
            picked[number % 4] = jnp.where(lane == number, turned, picked[number % 4])
        both = picked[0]
        for number in range(1, 4):
            both = jnp.where(lane % 4 == number, picked[number], both)
        part_of = (places_ref[pl.ds(block, 1), :] // LANES) % parts
        chosen = both
        for part in range(1, parts):
            chosen = jnp.where(part_of == part, pltpu.roll(both, ROWS - part * members, axis=0), chosen)
        mine_ref[pl.ds(block * members, members), :] = chosen[:members]
        return carry

    lax.fori_loop(0, blocks, gather, 0)
    for block in range(blocks):
        begin = (blocks + block) * members
        mine_ref[begin : begin + members, :] = noise_ref[:, block * LANES : (block + 1) * LANES]


def dot(a, b, contract, precision=HIGH):
    return lax.dot_general(a, b, (contract, ((), ())), precision=precision, preferred_element_type=jnp.float32)


def split_three(value):
    high = value.astype(jnp.bfloat16)
    rest = value - high.astype(jnp.float32)
    middle = rest.astype(jnp.bfloat16)
    return high, middle, (rest - middle.astype(jnp.float32)).astype(jnp.bfloat16)


def invert_all(matrix_ref):
    regions, size, _ = matrix_ref.shape
    lane = lanes_iota()
    row = rows_iota()

    def panel(number, carry):
        base = number * ROWS
        start = pl.multiple_of(base, ROWS)
        offset = lane - base
        inside = (offset >= 0) & (offset < ROWS)
        unit = jnp.where(offset == row, 1.0, 0.0)
        blocks = [matrix_ref[region, pl.ds(start, ROWS), :] for region in range(regions)]
        columns = []
        for k in range(ROWS):
            index = jnp.full((ROWS, LANES), base + k, jnp.int32)
            columns.append([jnp.take_along_axis(block, index, axis=1) for block in blocks])
        lefts = []
        for block in blocks:
            signed = jnp.where(inside, 0.0, jnp.where(offset < 0, block, -block))
            high, middle, low = split_three(signed)
            lefts.append(jnp.concatenate([high, high, middle, high, low, middle], axis=0))
        blocks = [jnp.where(inside, unit, block) for block in blocks]
        for j in range(ROWS):
            here = row == j
            for region in range(regions):
                pivot = columns[j][region]
                inverse = 1.0 / pivot[j : j + 1, :]
                scaled = blocks[region][j : j + 1, :] * inverse
                blocks[region] = jnp.where(here, scaled, blocks[region] - pivot * scaled)
                for k in range(j + 1, ROWS):
                    scaled = columns[k][region][j : j + 1, :] * inverse
                    columns[k][region] = jnp.where(here, scaled, columns[k][region] - pivot * scaled)
        for region in range(regions):
            high, middle, low = split_three(blocks[region])
            right = jnp.concatenate([high, middle, high, low, high, middle], axis=0)
            update = dot(lefts[region], right, ((0,), (0,)), lax.Precision.DEFAULT)
            for i in range(size // ROWS):
                rows = slice(i * ROWS, (i + 1) * ROWS)
                matrix_ref[region, rows, :] = jnp.where(inside, 0.0, matrix_ref[region, rows, :]) + update[rows]
            matrix_ref[region, pl.ds(start, ROWS), :] = blocks[region]
        return carry

    lax.fori_loop(0, size // ROWS, panel, 0)


def split_two(value):
    high = value.astype(jnp.bfloat16)
    return high, (value - high.astype(jnp.float32)).astype(jnp.bfloat16)


def dot_split(a, b, contract):
    a_high, a_low = split_two(a)
    b_high, b_low = split_two(b)
    low = dot(a_high, b_low, contract, lax.Precision.DEFAULT) + dot(a_low, b_high, contract, lax.Precision.DEFAULT)
    return dot(a_high, b_high, contract, lax.Precision.DEFAULT) + low


def prepare_kernel(zone_ref, neighbours_ref, variance_ref, places_ref, pick_ref, errors_ref, *, cells, zone_cells):
    regions, observations, size = pick_ref.shape
    ids = lax.broadcasted_iota(jnp.int32, (observations, size), 0)
    rows = jnp.concatenate([variance_ref[...], places_ref[...].astype(jnp.float32), jnp.zeros((ROWS - 2, observations), jnp.float32)])
    pieces = jnp.concatenate(split_three(rows))
    for region in range(regions):
        zone = zone_ref[0] + region
        pick = jnp.where(ids == neighbours_ref[pl.ds(zone, 1), :], 1.0, 0.0).astype(jnp.bfloat16)
        pick_ref[region, :, :] = pick
        picked = dot(pieces, pick, ((1,), (0,)), lax.Precision.DEFAULT)
        picked = picked[:ROWS] + picked[ROWS : 2 * ROWS] + picked[2 * ROWS :]
        centre = (zone * zone_cells + zone_cells // 2).astype(jnp.float32)
        gap = jnp.abs(picked[1:2] - centre)
        scaled = jnp.minimum(gap, cells - gap) / float(LSCALE)
        errors_ref[region : region + 1, :] = picked[0:1] * (1.0 + scaled * scaled)


def solve_kernel(me_ref, pick_ref, errors_ref, values_ref, variance_ref, *refs, masks):
    *blocks_refs, transform_ref, stack_ref, pieces_ref, matrix_ref = refs
    regions, total, _ = transform_ref.shape
    observations = values_ref.shape[1]
    blocks = observations // LANES
    members = blocks_refs[0].shape[1] // (2 * blocks)
    size = pick_ref.shape[2]
    for block in range(blocks):
        lanes = slice(block * LANES, (block + 1) * LANES)
        values = values_ref[:, lanes]
        spread = jnp.sqrt(variance_ref[:, lanes])
        for blocks_ref, mask in zip(blocks_refs, masks, strict=True):
            for number, bits in enumerate(mask):
                source = pl.multiple_of(lax.bitwise_xor(me_ref[0], bits) * members, members)
                equivalents = blocks_ref[number, block * members : (block + 1) * members, :]
                noise = blocks_ref[number, (blocks + block) * members : (blocks + block + 1) * members, :]
                stack_ref[block, pl.ds(source, members), :] = equivalents
                stack_ref[block, pl.ds(total + source, members), :] = values + spread * noise - equivalents
        for number, piece in enumerate(split_two(stack_ref[block])):
            pieces_ref[number * 2 * total : (number + 1) * 2 * total, lanes] = piece
    diagonal = lax.broadcasted_iota(jnp.int32, (size, size), 0) == lax.broadcasted_iota(jnp.int32, (size, size), 1)
    anomalies, innovations = [], []
    for region in range(regions):
        picked = dot(pieces_ref[...], pick_ref[region], ((1,), (0,)), lax.Precision.DEFAULT)
        picked = picked[: 2 * total] + picked[2 * total :]
        equivalents = picked[:total]
        innovations.append(picked[total:])
        anomaly = equivalents - jnp.sum(equivalents, axis=0, keepdims=True) * (1.0 / total)
        anomalies.append(anomaly)
        covariance = dot(anomaly, anomaly, ((0,), (0,))) * (1.0 / (total - 1))
        matrix_ref[region, :, :] = jnp.where(diagonal, covariance + errors_ref[region : region + 1, :], covariance)
    invert_all(matrix_ref)
    for region in range(regions):
        weights = dot_split(innovations[region], matrix_ref[region], ((1,), (0,)))
        transform_ref[region, :, :] = dot_split(weights, anomalies[region], ((1,), (1,))) * (1.0 / (total - 1))


def apply_kernel(counts_ref, transform_ref, cells_ref, owned_ref, block_ref, result_ref):
    sources, height, _ = cells_ref.shape
    regions, total, _ = transform_ref.shape
    members = total // sources
    tiles = height // members
    for tile in range(tiles):
        lanes = slice(tile * LANES, (tile + 1) * LANES)
        for source in range(sources):
            block_ref[source * members : (source + 1) * members, lanes] = cells_ref[source, tile * members : (tile + 1) * members, :]
    wide = tiles // regions
    for region in range(regions):
        block = block_ref[:, region * wide * LANES : (region + 1) * wide * LANES]
        anomalies = block - jnp.sum(block, axis=0, keepdims=True) * (1.0 / total)
        analysed = block + dot_split(transform_ref[region], anomalies, ((1,), (0,)))
        for place in range(wide):
            result_ref[region * wide + place, :total, :] = analysed[:, place * LANES : (place + 1) * LANES]
    for tile in range(tiles):
        result_ref[tile, total:, :] = jnp.zeros((ROWS, LANES), jnp.float32)

    def window(destination, offset):
        for tile in range(tiles):
            owned_ref[destination, tile * ROWS : (tile + 1) * ROWS, :] = result_ref[tile, pl.ds(offset, CAP), :]
        return offset + counts_ref[destination]

    lax.fori_loop(0, sources, window, jnp.int32(0))


def advance_kernel(count_ref, rows_ref, out_ref):
    sources, height, _ = rows_ref.shape
    tiles = height // ROWS
    here = out_ref.shape[1] // LANES // tiles
    lane = lanes_iota()
    occupied = rows_iota() < count_ref[0]
    start = pl.program_id(0) * here

    def load(source, tile):
        return rows_ref[source, tile * ROWS : (tile + 1) * ROWS, :]

    before = load(lax.rem(start + sources - 1, sources), tiles - 1)
    before_one = pltpu.roll(before, 1, axis=1)
    before_two = pltpu.roll(before, 2, axis=1)
    current = load(start, 0)
    current_up = pltpu.roll(current, LANES - 1, axis=1)
    for number in range(here * tiles):
        source, tile = divmod(number + 1, tiles)
        after = load(start + source if source < here else lax.rem(start + here, sources), tile)
        after_up = pltpu.roll(after, LANES - 1, axis=1)
        one = pltpu.roll(current, 1, axis=1)
        two = pltpu.roll(current, 2, axis=1)
        left = jnp.where(lane == 0, before_one, one)
        left_two = jnp.where(lane < 2, before_two, two)
        right = jnp.where(lane == LANES - 1, after_up, current_up)
        stepped = current + TIME_STEP * ((right - left_two) * left - current + FORCING)
        out_ref[:, number * LANES : (number + 1) * LANES] = jnp.where(occupied, stepped, 0.0)
        before_one, before_two = one, two
        current, current_up = after, after_up


def whole(space=pltpu.VMEM):
    return pl.BlockSpec(memory_space=space)


def in_vmem(value):
    return pltpu.with_memory_space_constraint(value, pltpu.VMEM)


def per_device(prior_sample_matrix, obs_values, obs_var, measured_indexes, neighbours, perturbation, counts):
    devices = lax.axis_size(AXES)
    depth = lax.axis_size("region")
    device_index = lax.axis_index(AXES)
    me = device_index.reshape(1)
    members, cells = prior_sample_matrix.shape
    total = members * devices
    observations = obs_values.shape[0]
    zones, local = neighbours.shape
    regions = zones // devices
    zone_cells = cells // zones
    blocks = observations // LANES
    share_tiles = cells // devices // LANES
    values = obs_values.reshape(1, observations)
    variance = obs_var.reshape(1, observations)

    def swap(value, bits):
        return lax.ppermute(value, AXES, [(device, device ^ bits) for device in range(devices)])

    exchange = functools.partial(lax.all_to_all, axis_name=AXES, split_axis=0, concat_axis=0, tiled=True)

    pick, errors = pl.pallas_call(
        functools.partial(prepare_kernel, cells=float(cells), zone_cells=zone_cells),
        out_shape=(
            jax.ShapeDtypeStruct((regions, observations, local), jnp.bfloat16),
            jax.ShapeDtypeStruct((regions, local), jnp.float32),
        ),
        in_specs=[whole(pltpu.SMEM), whole(), whole(), whole()],
        out_specs=(whole(),) * 2,
        name="prepare",
    )(me * regions, neighbours, variance, measured_indexes.reshape(1, observations))

    runs = prior_sample_matrix.reshape(members, cells // LANES, LANES).transpose(1, 0, 2).reshape(-1, LANES)
    height = runs.shape[0]
    tiles = height // LANES
    state, mine = pl.pallas_call(
        functools.partial(forecast_kernel, members=members),
        out_shape=(
            jax.ShapeDtypeStruct((height, LANES), jnp.float32),
            jax.ShapeDtypeStruct((2 * blocks * members, LANES), jnp.float32),
        ),
        in_specs=[whole()] * 3,
        out_specs=(whole(),) * 2,
        scratch_shapes=[
            pltpu.VMEM((max(tiles * (LANES + ROWS), LANES * (tiles + ROWS)), LANES), jnp.float32),
            pltpu.VMEM((2 * blocks, LANES), jnp.int32),
            pltpu.SMEM((2 * blocks, LANES), jnp.int32),
            pltpu.SemaphoreType.DMA,
        ],
        name="forecast",
    )(measured_indexes.reshape(blocks, LANES), perturbation, runs)

    near = mine[None]
    bits = 1
    while bits < depth:
        near = jnp.concatenate([near, swap(near, bits)])
        bits *= 2
    state, near = lax.optimization_barrier((state, near))
    own_cells = exchange(state.reshape(devices, height // devices, LANES))
    near_mask = list(range(depth))
    far_masks = [[chip * 2 * depth + bits for bits in near_mask] for chip in range(1, devices // (2 * depth))]
    far = [swap(near, mask[0]) for mask in far_masks]
    partner = swap(near, depth)
    partners = swap(jnp.concatenate(far), depth)
    pieces = [near, partner, *far, partners]
    masks = [near_mask, [depth ^ bits for bits in near_mask], *far_masks, [depth ^ bits for mask in far_masks for bits in mask]]

    transform = pl.pallas_call(
        functools.partial(solve_kernel, masks=masks),
        out_shape=jax.ShapeDtypeStruct((regions, total, total), jnp.float32),
        in_specs=[whole(pltpu.SMEM)] + [whole()] * (4 + len(pieces)),
        out_specs=whole(),
        scratch_shapes=[
            pltpu.VMEM((blocks, 2 * total, LANES), jnp.float32),
            pltpu.VMEM((4 * total, observations), jnp.bfloat16),
            pltpu.VMEM((regions, local, local), jnp.float32),
        ],
        name="solve",
    )(me, pick, errors, values, variance, *pieces)

    outgoing = pl.pallas_call(
        apply_kernel,
        out_shape=jax.ShapeDtypeStruct((devices, share_tiles * CAP, LANES), jnp.float32),
        in_specs=[whole(pltpu.SMEM), whole(), whole()],
        out_specs=whole(),
        scratch_shapes=[
            pltpu.VMEM((total, share_tiles * LANES), jnp.float32),
            pltpu.VMEM((share_tiles, total + ROWS, LANES), jnp.float32),
        ],
        name="analyse",
    )(counts, transform, in_vmem(own_cells))
    owned = exchange(outgoing)

    steps = 8
    return pl.pallas_call(
        advance_kernel,
        grid=(steps,),
        out_shape=jax.ShapeDtypeStruct((CAP, cells), jnp.float32),
        in_specs=[whole(pltpu.SMEM), whole()],
        out_specs=pl.BlockSpec((CAP, cells // steps), lambda i: (0, i)),
        name="advance",
    )(lax.dynamic_slice_in_dim(counts, device_index, 1, 0), in_vmem(owned))


def solution(mesh):
    rows = P(AXES, None)
    return jax.shard_map(
        per_device, mesh=mesh, in_specs=(rows, P(), P(), P(), P(), rows, P()), out_specs=rows, check_vma=False
    )
```

```python
import functools

import jax
import jax.numpy as jnp
from jax import lax
from jax.experimental import pallas as pl
from jax.experimental.pallas import tpu as pltpu
from jax.sharding import PartitionSpec as P


PREDICT_SUBTICKS = 24
CAP = 8
LSCALE = 2048
FORCING = 8.0
TIME_STEP = 0.01
HIGH = lax.Precision.HIGHEST
AXES = ("member", "region")
LANES = 128
VMEM_PIECES = 1 << 20
ROWS = 8


def lanes_iota():
    return lax.broadcasted_iota(jnp.int32, (ROWS, LANES), 1)


def rows_iota():
    return lax.broadcasted_iota(jnp.int32, (ROWS, LANES), 0)


def forecast_kernel(places_ref, noise_ref, x_ref, state_ref, mine_ref, tile_ref, table_ref, scalar_ref, table_sem, *, members):
    height = x_ref.shape[0]
    blocks = places_ref.shape[0]
    tiles = height // LANES
    halves = tiles // ROWS
    tile_pitch = LANES + ROWS
    cell_pitch = tiles + ROWS
    parts = ROWS // members
    lane = lanes_iota()
    row = rows_iota()

    def group(cell):
        return [state_ref[cell * tiles + half * ROWS : cell * tiles + (half + 1) * ROWS, :] for half in range(halves)]

    for tile in range(tiles):
        tile_ref[tile * tile_pitch : tile * tile_pitch + LANES, :] = (x_ref[tile * LANES : (tile + 1) * LANES, :] * TIME_STEP).T
    for cell in range(LANES):
        for half in range(halves):
            begin = cell * tiles + half * ROWS
            state_ref[begin : begin + ROWS, :] = tile_ref[pl.ds(half * ROWS * tile_pitch + cell, ROWS, stride=tile_pitch), :]

    places = places_ref[...]
    column = lax.broadcasted_iota(jnp.int32, places.shape, 1)
    table_ref[:blocks, :] = (places // (LANES * parts)) * ROWS
    table_ref[blocks:, :] = (column - places) & (LANES - 1)
    table_copy = pltpu.make_async_copy(table_ref, scalar_ref, table_sem)
    table_copy.start()

    def next_run(values):
        turned = [pltpu.roll(value, LANES - members, axis=1) for value in values]
        down = [pltpu.roll(value, ROWS - 1, axis=0) for value in turned]
        carried = [jnp.where(row == ROWS - 1, down[(half + 1) % halves], down[half]) for half in range(halves)]
        return [jnp.where(lane >= LANES - members, carry, value) for carry, value in zip(carried, turned, strict=True)]

    def previous_run(values):
        turned = [pltpu.roll(value, members, axis=1) for value in values]
        up = [pltpu.roll(value, 1, axis=0) for value in turned]
        carried = [jnp.where(row == 0, up[half - 1], up[half]) for half in range(halves)]
        return [jnp.where(lane < members, carry, value) for carry, value in zip(carried, turned, strict=True)]

    def advance(left_two, left, current, right):
        return [
            (c * (1.0 - TIME_STEP) + FORCING * TIME_STEP * TIME_STEP) + (d - a) * b
            for a, b, c, d in zip(left_two, left, current, right, strict=True)
        ]

    def store(cell, values):
        for half in range(halves):
            begin = cell * tiles + half * ROWS
            state_ref[begin : begin + ROWS, :] = values[half]

    def substep(_, carry):
        before_two = previous_run(group(LANES - 2))
        before = previous_run(group(LANES - 1))
        first = [group(cell) for cell in range(3)]
        beyond = next_run(first[0])
        window = list(first)
        for cell in range(2, LANES - 1):
            right = group(cell + 1)
            store(cell, advance(*window, right))
            window = window[1:] + [right]
        store(LANES - 1, advance(*window, beyond))
        store(0, advance(before_two, before, first[0], first[1]))
        store(1, advance(before, first[0], first[1], first[2]))
        return carry

    lax.fori_loop(0, PREDICT_SUBTICKS, substep, 0)

    for cell in range(LANES):
        for half in range(halves):
            begin = cell * cell_pitch + half * ROWS
            tile_ref[begin : begin + ROWS, :] = group(cell)[half]
    for tile in range(tiles):
        state_ref[tile * LANES : (tile + 1) * LANES, :] = tile_ref[pl.ds(tile, LANES, stride=cell_pitch), :].T * (1.0 / TIME_STEP)
    table_copy.wait()

    def gather(block, carry):
        picked = [jnp.zeros((ROWS, LANES), jnp.float32) for _ in range(4)]
        for number in range(LANES):
            begin = pl.multiple_of(scalar_ref[block, number], ROWS)
            turned = pltpu.roll(state_ref[pl.ds(begin, ROWS), :], scalar_ref[blocks + block, number], axis=1)
            picked[number % 4] = jnp.where(lane == number, turned, picked[number % 4])
        both = picked[0]
        for number in range(1, 4):
            both = jnp.where(lane % 4 == number, picked[number], both)
        part_of = (places_ref[pl.ds(block, 1), :] // LANES) % parts
        chosen = both
        for part in range(1, parts):
            chosen = jnp.where(part_of == part, pltpu.roll(both, ROWS - part * members, axis=0), chosen)
        mine_ref[pl.ds(block * members, members), :] = chosen[:members]
        return carry

    lax.fori_loop(0, blocks, gather, 0)
    for block in range(blocks):
        begin = (blocks + block) * members
        mine_ref[begin : begin + members, :] = noise_ref[:, block * LANES : (block + 1) * LANES]


def dot(a, b, contract, precision=HIGH):
    return lax.dot_general(a, b, (contract, ((), ())), precision=precision, preferred_element_type=jnp.float32)


def split_three(value):
    high = value.astype(jnp.bfloat16)
    rest = value - high.astype(jnp.float32)
    middle = rest.astype(jnp.bfloat16)
    return high, middle, (rest - middle.astype(jnp.float32)).astype(jnp.bfloat16)


def invert_all(matrix_ref):
    regions, size, _ = matrix_ref.shape
    lane = lanes_iota()
    row = rows_iota()

    def panel(number, carry):
        base = number * ROWS
        start = pl.multiple_of(base, ROWS)
        offset = lane - base
        inside = (offset >= 0) & (offset < ROWS)
        unit = jnp.where(offset == row, 1.0, 0.0)
        blocks = [matrix_ref[region, pl.ds(start, ROWS), :] for region in range(regions)]
        columns = []
        for k in range(ROWS):
            index = jnp.full((ROWS, LANES), base + k, jnp.int32)
            columns.append([jnp.take_along_axis(block, index, axis=1) for block in blocks])
        lefts = []
        for block in blocks:
            signed = jnp.where(inside, 0.0, jnp.where(offset < 0, block, -block))
            high, middle, low = split_three(signed)
            lefts.append(jnp.concatenate([high, high, middle, high, low, middle], axis=0))
        blocks = [jnp.where(inside, unit, block) for block in blocks]
        for j in range(ROWS):
            here = row == j
            for region in range(regions):
                pivot = columns[j][region]
                inverse = 1.0 / pivot[j : j + 1, :]
                scaled = blocks[region][j : j + 1, :] * inverse
                blocks[region] = jnp.where(here, scaled, blocks[region] - pivot * scaled)
                for k in range(j + 1, ROWS):
                    scaled = columns[k][region][j : j + 1, :] * inverse
                    columns[k][region] = jnp.where(here, scaled, columns[k][region] - pivot * scaled)
        for region in range(regions):
            high, middle, low = split_three(blocks[region])
            right = jnp.concatenate([high, middle, high, low, high, middle], axis=0)
            update = dot(lefts[region], right, ((0,), (0,)), lax.Precision.DEFAULT)
            for i in range(size // ROWS):
                rows = slice(i * ROWS, (i + 1) * ROWS)
                matrix_ref[region, rows, :] = jnp.where(inside, 0.0, matrix_ref[region, rows, :]) + update[rows]
            matrix_ref[region, pl.ds(start, ROWS), :] = blocks[region]
        return carry

    lax.fori_loop(0, size // ROWS, panel, 0)


def split_two(value):
    high = value.astype(jnp.bfloat16)
    return high, (value - high.astype(jnp.float32)).astype(jnp.bfloat16)


def dot_split(a, b, contract):
    a_high, a_low = split_two(a)
    b_high, b_low = split_two(b)
    low = dot(a_high, b_low, contract, lax.Precision.DEFAULT) + dot(a_low, b_high, contract, lax.Precision.DEFAULT)
    return dot(a_high, b_high, contract, lax.Precision.DEFAULT) + low


def prepare_kernel(zone_ref, neighbours_ref, variance_ref, places_ref, pick_ref, errors_ref, *, cells, zone_cells):
    regions, observations, size = pick_ref.shape
    ids = lax.broadcasted_iota(jnp.int32, (observations, size), 0)
    rows = jnp.concatenate([variance_ref[...], places_ref[...].astype(jnp.float32), jnp.zeros((ROWS - 2, observations), jnp.float32)])
    pieces = jnp.concatenate(split_three(rows))
    for region in range(regions):
        zone = zone_ref[0] + region
        pick = jnp.where(ids == neighbours_ref[pl.ds(zone, 1), :], 1.0, 0.0).astype(jnp.bfloat16)
        pick_ref[region, :, :] = pick
        picked = dot(pieces, pick, ((1,), (0,)), lax.Precision.DEFAULT)
        picked = picked[:ROWS] + picked[ROWS : 2 * ROWS] + picked[2 * ROWS :]
        centre = (zone * zone_cells + zone_cells // 2).astype(jnp.float32)
        gap = jnp.abs(picked[1:2] - centre)
        scaled = jnp.minimum(gap, cells - gap) / float(LSCALE)
        errors_ref[region : region + 1, :] = picked[0:1] * (1.0 + scaled * scaled)


def solve_kernel(me_ref, pick_ref, errors_ref, values_ref, variance_ref, *refs, masks):
    *blocks_refs, transform_ref, stack_ref, pieces_ref, matrix_ref = refs
    regions, total, _ = transform_ref.shape
    observations = values_ref.shape[1]
    blocks = observations // LANES
    members = blocks_refs[0].shape[1] // (2 * blocks)
    size = pick_ref.shape[2]
    for block in range(blocks):
        lanes = slice(block * LANES, (block + 1) * LANES)
        values = values_ref[:, lanes]
        spread = jnp.sqrt(variance_ref[:, lanes])
        for blocks_ref, mask in zip(blocks_refs, masks, strict=True):
            for number, bits in enumerate(mask):
                source = pl.multiple_of(lax.bitwise_xor(me_ref[0], bits) * members, members)
                equivalents = blocks_ref[number, block * members : (block + 1) * members, :]
                noise = blocks_ref[number, (blocks + block) * members : (blocks + block + 1) * members, :]
                stack_ref[block, pl.ds(source, members), :] = equivalents
                stack_ref[block, pl.ds(total + source, members), :] = values + spread * noise - equivalents
        for number, piece in enumerate(split_two(stack_ref[block])):
            pieces_ref[number * 2 * total : (number + 1) * 2 * total, lanes] = piece
    diagonal = lax.broadcasted_iota(jnp.int32, (size, size), 0) == lax.broadcasted_iota(jnp.int32, (size, size), 1)
    anomalies, innovations = [], []
    for region in range(regions):
        picked = dot(pieces_ref[...], pick_ref[region], ((1,), (0,)), lax.Precision.DEFAULT)
        picked = picked[: 2 * total] + picked[2 * total :]
        equivalents = picked[:total]
        innovations.append(picked[total:])
        anomaly = equivalents - jnp.sum(equivalents, axis=0, keepdims=True) * (1.0 / total)
        anomalies.append(anomaly)
        covariance = dot(anomaly, anomaly, ((0,), (0,))) * (1.0 / (total - 1))
        matrix_ref[region, :, :] = jnp.where(diagonal, covariance + errors_ref[region : region + 1, :], covariance)
    invert_all(matrix_ref)
    for region in range(regions):
        weights = dot_split(innovations[region], matrix_ref[region], ((1,), (0,)))
        transform_ref[region, :, :] = dot_split(weights, anomalies[region], ((1,), (1,))) * (1.0 / (total - 1))


def apply_kernel(counts_ref, transform_ref, cells_ref, owned_ref, block_ref, result_ref):
    sources, height, _ = cells_ref.shape
    regions, total, _ = transform_ref.shape
    members = total // sources
    tiles = height // members
    for tile in range(tiles):
        lanes = slice(tile * LANES, (tile + 1) * LANES)
        for source in range(sources):
            block_ref[source * members : (source + 1) * members, lanes] = cells_ref[source, tile * members : (tile + 1) * members, :]
    wide = tiles // regions
    for region in range(regions):
        block = block_ref[:, region * wide * LANES : (region + 1) * wide * LANES]
        anomalies = block - jnp.sum(block, axis=0, keepdims=True) * (1.0 / total)
        analysed = block + dot_split(transform_ref[region], anomalies, ((1,), (0,)))
        for place in range(wide):
            result_ref[region * wide + place, :total, :] = analysed[:, place * LANES : (place + 1) * LANES]
    for tile in range(tiles):
        result_ref[tile, total:, :] = jnp.zeros((ROWS, LANES), jnp.float32)

    def window(destination, offset):
        for tile in range(tiles):
            owned_ref[destination, tile * ROWS : (tile + 1) * ROWS, :] = result_ref[tile, pl.ds(offset, CAP), :]
        return offset + counts_ref[destination]

    lax.fori_loop(0, sources, window, jnp.int32(0))


def advance_kernel(count_ref, rows_ref, out_ref):
    sources, height, _ = rows_ref.shape
    tiles = height // ROWS
    here = out_ref.shape[1] // LANES // tiles
    lane = lanes_iota()
    occupied = rows_iota() < count_ref[0]
    start = pl.program_id(0) * here

    def load(source, tile):
        return rows_ref[source, tile * ROWS : (tile + 1) * ROWS, :]

    before = load(lax.rem(start + sources - 1, sources), tiles - 1)
    before_one = pltpu.roll(before, 1, axis=1)
    before_two = pltpu.roll(before, 2, axis=1)
    current = load(start, 0)
    current_up = pltpu.roll(current, LANES - 1, axis=1)
    for number in range(here * tiles):
        source, tile = divmod(number + 1, tiles)
        after = load(start + source if source < here else lax.rem(start + here, sources), tile)
        after_up = pltpu.roll(after, LANES - 1, axis=1)
        one = pltpu.roll(current, 1, axis=1)
        two = pltpu.roll(current, 2, axis=1)
        left = jnp.where(lane == 0, before_one, one)
        left_two = jnp.where(lane < 2, before_two, two)
        right = jnp.where(lane == LANES - 1, after_up, current_up)
        stepped = current + TIME_STEP * ((right - left_two) * left - current + FORCING)
        out_ref[:, number * LANES : (number + 1) * LANES] = jnp.where(occupied, stepped, 0.0)
        before_one, before_two = one, two
        current, current_up = after, after_up


def whole(space=pltpu.VMEM):
    return pl.BlockSpec(memory_space=space)


def in_vmem(value):
    return pltpu.with_memory_space_constraint(value, pltpu.VMEM)


def per_device(prior_sample_matrix, obs_values, obs_var, measured_indexes, neighbours, perturbation, counts):
    devices = lax.axis_size(AXES)
    depth = lax.axis_size("region")
    device_index = lax.axis_index(AXES)
    me = device_index.reshape(1)
    members, cells = prior_sample_matrix.shape
    total = members * devices
    observations = obs_values.shape[0]
    zones, local = neighbours.shape
    regions = zones // devices
    zone_cells = cells // zones
    blocks = observations // LANES
    share_tiles = cells // devices // LANES
    values = obs_values.reshape(1, observations)
    variance = obs_var.reshape(1, observations)

    def swap(value, bits):
        return lax.ppermute(value, AXES, [(device, device ^ bits) for device in range(devices)])

    exchange = functools.partial(lax.all_to_all, axis_name=AXES, split_axis=0, concat_axis=0, tiled=True)

    pick, errors = pl.pallas_call(
        functools.partial(prepare_kernel, cells=float(cells), zone_cells=zone_cells),
        out_shape=(
            jax.ShapeDtypeStruct((regions, observations, local), jnp.bfloat16),
            jax.ShapeDtypeStruct((regions, local), jnp.float32),
        ),
        in_specs=[whole(pltpu.SMEM), whole(), whole(), whole()],
        out_specs=(whole(),) * 2,
        name="prepare",
    )(me * regions, neighbours, variance, measured_indexes.reshape(1, observations))

    runs = prior_sample_matrix.reshape(members, cells // LANES, LANES).transpose(1, 0, 2).reshape(-1, LANES)
    height = runs.shape[0]
    tiles = height // LANES
    state, mine = pl.pallas_call(
        functools.partial(forecast_kernel, members=members),
        out_shape=(
            jax.ShapeDtypeStruct((height, LANES), jnp.float32),
            jax.ShapeDtypeStruct((2 * blocks * members, LANES), jnp.float32),
        ),
        in_specs=[whole()] * 3,
        out_specs=(whole(),) * 2,
        scratch_shapes=[
            pltpu.VMEM((max(tiles * (LANES + ROWS), LANES * (tiles + ROWS)), LANES), jnp.float32),
            pltpu.VMEM((2 * blocks, LANES), jnp.int32),
            pltpu.SMEM((2 * blocks, LANES), jnp.int32),
            pltpu.SemaphoreType.DMA,
        ],
        name="forecast",
    )(measured_indexes.reshape(blocks, LANES), perturbation, runs)

    near = jnp.concatenate([mine[None]] + [swap(mine[None], bits) for bits in range(1, depth)])
    near_mask = list(range(depth))
    far_masks = [[chip * 2 * depth + bits for bits in near_mask] for chip in range(1, devices // (2 * depth))]
    far = []
    for mask in far_masks:
        far.append(swap(near, mask[0]))
    state, near = lax.optimization_barrier((state, near))
    own_cells = exchange(state.reshape(devices, height // devices, LANES))
    partner = swap(near, depth)
    partners = swap(jnp.concatenate(far), depth)
    pieces = [near, partner, *far, partners]
    masks = [near_mask, [depth ^ bits for bits in near_mask], *far_masks, [depth ^ bits for mask in far_masks for bits in mask]]

    place = in_vmem if sum(piece.size for piece in pieces) * 4 <= VMEM_PIECES else lambda value: value
    transform = pl.pallas_call(
        functools.partial(solve_kernel, masks=masks),
        out_shape=jax.ShapeDtypeStruct((regions, total, total), jnp.float32),
        in_specs=[whole(pltpu.SMEM)] + [whole()] * (4 + len(pieces)),
        out_specs=whole(),
        scratch_shapes=[
            pltpu.VMEM((blocks, 2 * total, LANES), jnp.float32),
            pltpu.VMEM((4 * total, observations), jnp.bfloat16),
            pltpu.VMEM((regions, local, local), jnp.float32),
        ],
        name="solve",
    )(me, pick, errors, values, variance, *map(place, pieces))

    outgoing = pl.pallas_call(
        apply_kernel,
        out_shape=jax.ShapeDtypeStruct((devices, share_tiles * CAP, LANES), jnp.float32),
        in_specs=[whole(pltpu.SMEM), whole(), whole()],
        out_specs=whole(),
        scratch_shapes=[
            pltpu.VMEM((total, share_tiles * LANES), jnp.float32),
            pltpu.VMEM((share_tiles, total + ROWS, LANES), jnp.float32),
        ],
        name="analyse",
    )(counts, transform, in_vmem(own_cells))
    owned = exchange(outgoing)

    steps = 4
    return pl.pallas_call(
        advance_kernel,
        grid=(steps,),
        out_shape=jax.ShapeDtypeStruct((CAP, cells), jnp.float32),
        in_specs=[whole(pltpu.SMEM), whole()],
        out_specs=pl.BlockSpec((CAP, cells // steps), lambda i: (0, i)),
        name="advance",
    )(lax.dynamic_slice_in_dim(counts, device_index, 1, 0), in_vmem(owned))


def solution(mesh):
    rows = P(AXES, None)
    return jax.shard_map(
        per_device, mesh=mesh, in_specs=(rows, P(), P(), P(), P(), rows, P()), out_specs=rows, check_vma=False
    )
```

```python
import functools

import jax
import jax.numpy as jnp
from jax import lax
from jax.experimental import pallas as pl
from jax.experimental.pallas import tpu as pltpu
from jax.sharding import PartitionSpec as P


PREDICT_SUBTICKS = 24
CAP = 8
LSCALE = 2048
FORCING = 8.0
TIME_STEP = 0.01
HIGH = lax.Precision.HIGHEST
AXES = ("member", "region")
LANES = 128
VMEM_PIECES = 1 << 20
ROWS = 8


def lanes_iota():
    return lax.broadcasted_iota(jnp.int32, (ROWS, LANES), 1)


def rows_iota():
    return lax.broadcasted_iota(jnp.int32, (ROWS, LANES), 0)


def forecast_kernel(places_ref, noise_ref, x_ref, out_ref, mine_ref, rows_ref, state_ref, tile_ref, table_ref, scalar_ref, table_sem, in_sem, out_sem, *, members):
    height = x_ref.shape[0]
    blocks = places_ref.shape[0]
    tiles = height // LANES
    halves = tiles // ROWS
    tile_pitch = LANES + ROWS
    cell_pitch = tiles + ROWS
    parts = ROWS // members
    lane = lanes_iota()
    row = rows_iota()

    def group(cell):
        return [state_ref[cell * tiles + half * ROWS : cell * tiles + (half + 1) * ROWS, :] for half in range(halves)]

    def tile_rows(tile):
        return slice(tile * LANES, (tile + 1) * LANES)

    incoming = [pltpu.make_async_copy(x_ref.at[tile_rows(tile)], rows_ref.at[tile_rows(tile)], in_sem.at[tile]) for tile in range(tiles)]
    for copy in incoming:
        copy.start()
    for tile, copy in enumerate(incoming):
        copy.wait()
        tile_ref[tile * tile_pitch : tile * tile_pitch + LANES, :] = (rows_ref[tile_rows(tile), :] * TIME_STEP).T
    for cell in range(LANES):
        for half in range(halves):
            begin = cell * tiles + half * ROWS
            state_ref[begin : begin + ROWS, :] = tile_ref[pl.ds(half * ROWS * tile_pitch + cell, ROWS, stride=tile_pitch), :]

    places = places_ref[...]
    column = lax.broadcasted_iota(jnp.int32, places.shape, 1)
    table_ref[:blocks, :] = (places // (LANES * parts)) * ROWS
    table_ref[blocks:, :] = (column - places) & (LANES - 1)
    table_copy = pltpu.make_async_copy(table_ref, scalar_ref, table_sem)
    table_copy.start()

    def next_run(values):
        turned = [pltpu.roll(value, LANES - members, axis=1) for value in values]
        down = [pltpu.roll(value, ROWS - 1, axis=0) for value in turned]
        carried = [jnp.where(row == ROWS - 1, down[(half + 1) % halves], down[half]) for half in range(halves)]
        return [jnp.where(lane >= LANES - members, carry, value) for carry, value in zip(carried, turned, strict=True)]

    def previous_run(values):
        turned = [pltpu.roll(value, members, axis=1) for value in values]
        up = [pltpu.roll(value, 1, axis=0) for value in turned]
        carried = [jnp.where(row == 0, up[half - 1], up[half]) for half in range(halves)]
        return [jnp.where(lane < members, carry, value) for carry, value in zip(carried, turned, strict=True)]

    def advance(left_two, left, current, right):
        return [
            (c * (1.0 - TIME_STEP) + FORCING * TIME_STEP * TIME_STEP) + (d - a) * b
            for a, b, c, d in zip(left_two, left, current, right, strict=True)
        ]

    def store(cell, values):
        for half in range(halves):
            begin = cell * tiles + half * ROWS
            state_ref[begin : begin + ROWS, :] = values[half]

    def substep(_, carry):
        before_two = previous_run(group(LANES - 2))
        before = previous_run(group(LANES - 1))
        first = [group(cell) for cell in range(3)]
        beyond = next_run(first[0])
        window = list(first)
        for cell in range(2, LANES - 1):
            right = group(cell + 1)
            store(cell, advance(*window, right))
            window = window[1:] + [right]
        store(LANES - 1, advance(*window, beyond))
        store(0, advance(before_two, before, first[0], first[1]))
        store(1, advance(before, first[0], first[1], first[2]))
        return carry

    lax.fori_loop(0, PREDICT_SUBTICKS, substep, 0)

    for cell in range(LANES):
        for half in range(halves):
            begin = cell * cell_pitch + half * ROWS
            tile_ref[begin : begin + ROWS, :] = group(cell)[half]
    outgoing = [pltpu.make_async_copy(rows_ref.at[tile_rows(tile)], out_ref.at[tile_rows(tile)], out_sem.at[tile]) for tile in range(tiles)]
    for tile, copy in enumerate(outgoing):
        rows_ref[tile_rows(tile), :] = tile_ref[pl.ds(tile, LANES, stride=cell_pitch), :].T * (1.0 / TIME_STEP)
        copy.start()
    table_copy.wait()

    def gather(block, carry):
        picked = [jnp.zeros((ROWS, LANES), jnp.float32) for _ in range(4)]
        for number in range(LANES):
            begin = pl.multiple_of(scalar_ref[block, number], ROWS)
            turned = pltpu.roll(rows_ref[pl.ds(begin, ROWS), :], scalar_ref[blocks + block, number], axis=1)
            picked[number % 4] = jnp.where(lane == number, turned, picked[number % 4])
        both = picked[0]
        for number in range(1, 4):
            both = jnp.where(lane % 4 == number, picked[number], both)
        part_of = (places_ref[pl.ds(block, 1), :] // LANES) % parts
        chosen = both
        for part in range(1, parts):
            chosen = jnp.where(part_of == part, pltpu.roll(both, ROWS - part * members, axis=0), chosen)
        mine_ref[pl.ds(block * members, members), :] = chosen[:members]
        return carry

    lax.fori_loop(0, blocks, gather, 0)
    for block in range(blocks):
        begin = (blocks + block) * members
        mine_ref[begin : begin + members, :] = noise_ref[:, block * LANES : (block + 1) * LANES]
    for copy in outgoing:
        copy.wait()


def dot(a, b, contract, precision=HIGH):
    return lax.dot_general(a, b, (contract, ((), ())), precision=precision, preferred_element_type=jnp.float32)


def split_three(value):
    high = value.astype(jnp.bfloat16)
    rest = value - high.astype(jnp.float32)
    middle = rest.astype(jnp.bfloat16)
    return high, middle, (rest - middle.astype(jnp.float32)).astype(jnp.bfloat16)


def invert_all(matrix_refs, left_refs, right_refs, done_refs):
    regions = len(matrix_refs)
    size = matrix_refs[0].shape[0]
    panels = size // ROWS
    lane = lanes_iota()
    row = rows_iota()

    def inside(number):
        offset = lane - number * ROWS
        return (offset >= 0) & (offset < ROWS)

    def rows_of(number):
        return pl.ds(pl.multiple_of(number * ROWS, ROWS), ROWS)

    def add_products(group, number):
        for region in group:
            update = dot(left_refs[region][...], right_refs[region][...], ((0,), (0,)), lax.Precision.DEFAULT)
            for i in range(panels):
                rows = slice(i * ROWS, (i + 1) * ROWS)
                matrix_refs[region][rows, :] = jnp.where(inside(number), 0.0, matrix_refs[region][rows, :]) + update[rows]
            matrix_refs[region][rows_of(number), :] = done_refs[region][...]

    def eliminate(group, number):
        offset = lane - number * ROWS
        here = inside(number)
        unit = jnp.where(offset == row, 1.0, 0.0)
        blocks = {region: matrix_refs[region][rows_of(number), :] for region in group}
        columns = []
        for k in range(ROWS):
            index = jnp.full((ROWS, LANES), number * ROWS + k, jnp.int32)
            columns.append({region: jnp.take_along_axis(blocks[region], index, axis=1) for region in group})
        for region in group:
            high, middle, low = split_three(jnp.where(here, 0.0, jnp.where(offset < 0, blocks[region], -blocks[region])))
            left_refs[region][...] = jnp.concatenate([high, high, middle, high, low, middle], axis=0)
            blocks[region] = jnp.where(here, unit, blocks[region])
        for j in range(ROWS):
            at = row == j
            for region in group:
                pivot = columns[j][region]
                inverse = 1.0 / pivot[j : j + 1, :]
                scaled = blocks[region][j : j + 1, :] * inverse
                blocks[region] = jnp.where(at, scaled, blocks[region] - pivot * scaled)
                for k in range(j + 1, ROWS):
                    scaled = columns[k][region][j : j + 1, :] * inverse
                    columns[k][region] = jnp.where(at, scaled, columns[k][region] - pivot * scaled)
        for region in group:
            done_refs[region][...] = blocks[region]
            high, middle, low = split_three(blocks[region])
            right_refs[region][...] = jnp.concatenate([high, middle, high, low, high, middle], axis=0)

    def panel(number, carry):
        eliminate(range(regions), number)
        add_products(range(regions), number)
        return carry

    lax.fori_loop(0, panels, panel, 0)


def invert_scratch(regions, size):
    factor = pltpu.VMEM((6 * ROWS, size), jnp.bfloat16)
    return [[pltpu.VMEM((size, size), jnp.float32)] * regions, [factor] * regions, [factor] * regions, [pltpu.VMEM((ROWS, size), jnp.float32)] * regions]


def split_two(value):
    high = value.astype(jnp.bfloat16)
    return high, (value - high.astype(jnp.float32)).astype(jnp.bfloat16)


def dot_split(a, b, contract):
    a_high, a_low = split_two(a)
    b_high, b_low = split_two(b)
    low = dot(a_high, b_low, contract, lax.Precision.DEFAULT) + dot(a_low, b_high, contract, lax.Precision.DEFAULT)
    return dot(a_high, b_high, contract, lax.Precision.DEFAULT) + low


def prepare_kernel(zone_ref, neighbours_ref, variance_ref, places_ref, pick_ref, errors_ref, *, cells, zone_cells):
    regions, observations, size = pick_ref.shape
    ids = lax.broadcasted_iota(jnp.int32, (observations, size), 0)
    rows = jnp.concatenate([variance_ref[...], places_ref[...].astype(jnp.float32), jnp.zeros((ROWS - 2, observations), jnp.float32)])
    pieces = jnp.concatenate(split_three(rows))
    for region in range(regions):
        zone = zone_ref[0] + region
        pick = jnp.where(ids == neighbours_ref[pl.ds(zone, 1), :], 1.0, 0.0).astype(jnp.bfloat16)
        pick_ref[region, :, :] = pick
        picked = dot(pieces, pick, ((1,), (0,)), lax.Precision.DEFAULT)
        picked = picked[:ROWS] + picked[ROWS : 2 * ROWS] + picked[2 * ROWS :]
        centre = (zone * zone_cells + zone_cells // 2).astype(jnp.float32)
        gap = jnp.abs(picked[1:2] - centre)
        scaled = jnp.minimum(gap, cells - gap) / float(LSCALE)
        errors_ref[region : region + 1, :] = picked[0:1] * (1.0 + scaled * scaled)


def solve_kernel(me_ref, pick_ref, errors_ref, values_ref, variance_ref, *refs, masks):
    *blocks_refs, transform_ref, stack_ref, pieces_ref, matrix_refs, left_refs, right_refs, done_refs = refs
    regions, total, _ = transform_ref.shape
    observations = values_ref.shape[1]
    blocks = observations // LANES
    members = blocks_refs[0].shape[1] // (2 * blocks)
    size = pick_ref.shape[2]
    for block in range(blocks):
        lanes = slice(block * LANES, (block + 1) * LANES)
        values = values_ref[:, lanes]
        spread = jnp.sqrt(variance_ref[:, lanes])
        for blocks_ref, mask in zip(blocks_refs, masks, strict=True):
            for number, bits in enumerate(mask):
                source = pl.multiple_of(lax.bitwise_xor(me_ref[0], bits) * members, members)
                equivalents = blocks_ref[number, block * members : (block + 1) * members, :]
                noise = blocks_ref[number, (blocks + block) * members : (blocks + block + 1) * members, :]
                stack_ref[block, pl.ds(source, members), :] = equivalents
                stack_ref[block, pl.ds(total + source, members), :] = values + spread * noise - equivalents
        for number, piece in enumerate(split_two(stack_ref[block])):
            pieces_ref[number * 2 * total : (number + 1) * 2 * total, lanes] = piece
    diagonal = lax.broadcasted_iota(jnp.int32, (size, size), 0) == lax.broadcasted_iota(jnp.int32, (size, size), 1)
    anomalies, innovations = [], []
    for region in range(regions):
        picked = dot(pieces_ref[...], pick_ref[region], ((1,), (0,)), lax.Precision.DEFAULT)
        picked = picked[: 2 * total] + picked[2 * total :]
        equivalents = picked[:total]
        innovations.append(picked[total:])
        anomaly = equivalents - jnp.sum(equivalents, axis=0, keepdims=True) * (1.0 / total)
        anomalies.append(anomaly)
        covariance = dot(anomaly.T, anomaly, ((1,), (0,))) * (1.0 / (total - 1))
        matrix_refs[region][...] = jnp.where(diagonal, covariance + errors_ref[region : region + 1, :], covariance)
    invert_all(matrix_refs, left_refs, right_refs, done_refs)
    for region in range(regions):
        weights = dot_split(innovations[region], matrix_refs[region][...], ((1,), (0,)))
        transform_ref[region, :, :] = dot_split(weights, anomalies[region], ((1,), (1,))) * (1.0 / (total - 1))


def apply_kernel(counts_ref, transform_ref, cells_ref, owned_ref, block_ref, result_ref, staging_ref, out_sem):
    sources, height, _ = cells_ref.shape
    regions, total, _ = transform_ref.shape
    members = total // sources
    tiles = height // members
    for tile in range(tiles):
        lanes = slice(tile * LANES, (tile + 1) * LANES)
        for source in range(sources):
            block_ref[source * members : (source + 1) * members, lanes] = cells_ref[source, tile * members : (tile + 1) * members, :]
    wide = tiles // regions
    for region in range(regions):
        block = block_ref[:, region * wide * LANES : (region + 1) * wide * LANES]
        anomalies = block - jnp.sum(block, axis=0, keepdims=True) * (1.0 / total)
        analysed = block + dot_split(transform_ref[region], anomalies, ((1,), (0,)))
        for place in range(wide):
            result_ref[region * wide + place, :total, :] = analysed[:, place * LANES : (place + 1) * LANES]
    for tile in range(tiles):
        result_ref[tile, total:, :] = jnp.zeros((ROWS, LANES), jnp.float32)

    def window(destination, offset):
        for tile in range(tiles):
            staging_ref[destination, tile * ROWS : (tile + 1) * ROWS, :] = result_ref[tile, pl.ds(offset, CAP), :]
        return offset + counts_ref[destination]

    groups = out_sem.shape[0]
    group = sources // groups
    offset = jnp.int32(0)
    copies = []
    for number in range(groups):
        offset = lax.fori_loop(number * group, (number + 1) * group, window, offset)
        span = slice(number * group, (number + 1) * group)
        copies.append(pltpu.make_async_copy(staging_ref.at[span], owned_ref.at[span], out_sem.at[number]))
        copies[-1].start()
    for copy in copies:
        copy.wait()


def advance_kernel(count_ref, rows_ref, out_ref, staging_ref, out_sem):
    sources, height, _ = rows_ref.shape
    tiles = height // ROWS
    chunks = out_sem.shape[0]
    here = sources // chunks
    width = here * tiles * LANES
    lane = lanes_iota()
    occupied = rows_iota() < count_ref[0]

    def load(source, tile):
        return rows_ref[source, tile * ROWS : (tile + 1) * ROWS, :]

    def out_copy(chunk):
        lanes = pl.ds(pl.multiple_of(chunk * width, width), width)
        return pltpu.make_async_copy(staging_ref.at[chunk], out_ref.at[:, lanes], out_sem.at[chunk])

    def step(chunk, carry):
        start = chunk * here
        before = load(lax.rem(start + sources - 1, sources), tiles - 1)
        before_one = pltpu.roll(before, 1, axis=1)
        before_two = pltpu.roll(before, 2, axis=1)
        current = load(start, 0)
        current_up = pltpu.roll(current, LANES - 1, axis=1)
        for number in range(here * tiles):
            source, tile = divmod(number + 1, tiles)
            after = load(start + source if source < here else lax.rem(start + here, sources), tile)
            after_up = pltpu.roll(after, LANES - 1, axis=1)
            one = pltpu.roll(current, 1, axis=1)
            two = pltpu.roll(current, 2, axis=1)
            left = jnp.where(lane == 0, before_one, one)
            left_two = jnp.where(lane < 2, before_two, two)
            right = jnp.where(lane == LANES - 1, after_up, current_up)
            stepped = current + TIME_STEP * ((right - left_two) * left - current + FORCING)
            staging_ref[chunk, :, number * LANES : (number + 1) * LANES] = jnp.where(occupied, stepped, 0.0)
            before_one, before_two = one, two
            current, current_up = after, after_up
        out_copy(chunk).start()
        return carry

    lax.fori_loop(0, chunks, step, 0)
    for chunk in range(chunks):
        out_copy(chunk).wait()


def whole(space=pltpu.VMEM):
    return pl.BlockSpec(memory_space=space)


def in_vmem(value):
    return pltpu.with_memory_space_constraint(value, pltpu.VMEM)


def per_device(prior_sample_matrix, obs_values, obs_var, measured_indexes, neighbours, perturbation, counts):
    devices = lax.axis_size(AXES)
    depth = lax.axis_size("region")
    device_index = lax.axis_index(AXES)
    me = device_index.reshape(1)
    members, cells = prior_sample_matrix.shape
    total = members * devices
    observations = obs_values.shape[0]
    zones, local = neighbours.shape
    regions = zones // devices
    zone_cells = cells // zones
    blocks = observations // LANES
    share_tiles = cells // devices // LANES
    values = obs_values.reshape(1, observations)
    variance = obs_var.reshape(1, observations)

    def swap(value, bits):
        return lax.ppermute(value, AXES, [(device, device ^ bits) for device in range(devices)])

    exchange = functools.partial(lax.all_to_all, axis_name=AXES, split_axis=0, concat_axis=0, tiled=True)

    pick, errors = pl.pallas_call(
        functools.partial(prepare_kernel, cells=float(cells), zone_cells=zone_cells),
        out_shape=(
            jax.ShapeDtypeStruct((regions, observations, local), jnp.bfloat16),
            jax.ShapeDtypeStruct((regions, local), jnp.float32),
        ),
        in_specs=[whole(pltpu.SMEM), whole(), whole(), whole()],
        out_specs=(whole(),) * 2,
        name="prepare",
    )(me * regions, neighbours, variance, measured_indexes.reshape(1, observations))

    runs = prior_sample_matrix.reshape(members, cells // LANES, LANES).transpose(1, 0, 2).reshape(-1, LANES)
    height = runs.shape[0]
    tiles = height // LANES
    state, mine = pl.pallas_call(
        functools.partial(forecast_kernel, members=members),
        out_shape=(
            jax.ShapeDtypeStruct((height, LANES), jnp.float32),
            jax.ShapeDtypeStruct((2 * blocks * members, LANES), jnp.float32),
        ),
        in_specs=[whole(), whole(), whole(pltpu.HBM)],
        out_specs=(whole(pltpu.HBM), whole()),
        scratch_shapes=[
            pltpu.VMEM((height, LANES), jnp.float32),
            pltpu.VMEM((height, LANES), jnp.float32),
            pltpu.VMEM((max(tiles * (LANES + ROWS), LANES * (tiles + ROWS)), LANES), jnp.float32),
            pltpu.VMEM((2 * blocks, LANES), jnp.int32),
            pltpu.SMEM((2 * blocks, LANES), jnp.int32),
            pltpu.SemaphoreType.DMA,
            pltpu.SemaphoreType.DMA((tiles,)),
            pltpu.SemaphoreType.DMA((tiles,)),
        ],
        name="forecast",
    )(measured_indexes.reshape(blocks, LANES), perturbation, runs)

    near = jnp.concatenate([mine[None]] + [swap(mine[None], bits) for bits in range(1, depth)])
    near_mask = list(range(depth))
    far_masks = [[chip * 2 * depth + bits for bits in near_mask] for chip in range(1, devices // (2 * depth))]
    far = []
    for mask in far_masks:
        far.append(swap(near, mask[0]))
    state, near = lax.optimization_barrier((state, near))
    own_cells = exchange(state.reshape(devices, height // devices, LANES))
    partner = swap(near, depth)
    partners = swap(jnp.concatenate(far), depth)
    pieces = [near, partner, *far, partners]
    masks = [near_mask, [depth ^ bits for bits in near_mask], *far_masks, [depth ^ bits for mask in far_masks for bits in mask]]

    place = in_vmem if sum(piece.size for piece in pieces) * 4 <= VMEM_PIECES else lambda value: value
    transform = pl.pallas_call(
        functools.partial(solve_kernel, masks=masks),
        out_shape=jax.ShapeDtypeStruct((regions, total, total), jnp.float32),
        in_specs=[whole(pltpu.SMEM)] + [whole()] * (4 + len(pieces)),
        out_specs=whole(),
        scratch_shapes=[
            pltpu.VMEM((blocks, 2 * total, LANES), jnp.float32),
            pltpu.VMEM((4 * total, observations), jnp.bfloat16),
            *invert_scratch(regions, local),
        ],
        name="solve",
    )(me, pick, errors, values, variance, *map(place, pieces))

    outgoing = pl.pallas_call(
        apply_kernel,
        out_shape=jax.ShapeDtypeStruct((devices, share_tiles * CAP, LANES), jnp.float32),
        in_specs=[whole(pltpu.SMEM), whole(), whole()],
        out_specs=whole(pltpu.HBM),
        scratch_shapes=[
            pltpu.VMEM((total, share_tiles * LANES), jnp.float32),
            pltpu.VMEM((share_tiles, total + ROWS, LANES), jnp.float32),
            pltpu.VMEM((devices, share_tiles * CAP, LANES), jnp.float32),
            pltpu.SemaphoreType.DMA((4,)),
        ],
        name="analyse",
    )(counts, transform, in_vmem(own_cells))
    owned = exchange(outgoing)

    chunks = 8
    return pl.pallas_call(
        advance_kernel,
        out_shape=jax.ShapeDtypeStruct((CAP, cells), jnp.float32),
        in_specs=[whole(pltpu.SMEM), whole()],
        out_specs=whole(pltpu.HBM),
        scratch_shapes=[pltpu.VMEM((chunks, CAP, cells // chunks), jnp.float32), pltpu.SemaphoreType.DMA((chunks,))],
        name="advance",
    )(lax.dynamic_slice_in_dim(counts, device_index, 1, 0), in_vmem(owned))


def solution(mesh):
    rows = P(AXES, None)
    return jax.shard_map(
        per_device, mesh=mesh, in_specs=(rows, P(), P(), P(), P(), rows, P()), out_specs=rows, check_vma=False
    )
```

```python
import functools

import jax
import jax.numpy as jnp
from jax import lax
from jax.experimental import pallas as pl
from jax.experimental.pallas import tpu as pltpu
from jax.sharding import PartitionSpec as P


PREDICT_SUBTICKS = 24
CAP = 8
LSCALE = 2048
FORCING = 8.0
TIME_STEP = 0.01
HIGH = lax.Precision.HIGHEST
AXES = ("member", "region")
LANES = 128
VMEM_PIECES = 1 << 20
ROWS = 8


def lanes_iota():
    return lax.broadcasted_iota(jnp.int32, (ROWS, LANES), 1)


def rows_iota():
    return lax.broadcasted_iota(jnp.int32, (ROWS, LANES), 0)


def forecast_kernel(places_ref, noise_ref, x_ref, out_ref, mine_ref, rows_ref, state_ref, tile_ref, table_ref, scalar_ref, table_sem, out_sem, *, members):
    height = x_ref.shape[0]
    blocks = places_ref.shape[0]
    tiles = height // LANES
    halves = tiles // ROWS
    tile_pitch = LANES + ROWS
    cell_pitch = tiles + ROWS
    parts = ROWS // members
    lane = lanes_iota()
    row = rows_iota()

    def group(cell):
        return [state_ref[cell * tiles + half * ROWS : cell * tiles + (half + 1) * ROWS, :] for half in range(halves)]

    def tile_rows(tile):
        return slice(tile * LANES, (tile + 1) * LANES)

    for tile in range(tiles):
        tile_ref[tile * tile_pitch : tile * tile_pitch + LANES, :] = (x_ref[tile_rows(tile), :] * TIME_STEP).T
    for cell in range(LANES):
        for half in range(halves):
            begin = cell * tiles + half * ROWS
            state_ref[begin : begin + ROWS, :] = tile_ref[pl.ds(half * ROWS * tile_pitch + cell, ROWS, stride=tile_pitch), :]

    places = places_ref[...]
    column = lax.broadcasted_iota(jnp.int32, places.shape, 1)
    table_ref[:blocks, :] = (places // (LANES * parts)) * ROWS
    table_ref[blocks:, :] = (column - places) & (LANES - 1)
    table_copy = pltpu.make_async_copy(table_ref, scalar_ref, table_sem)
    table_copy.start()

    def next_run(values):
        turned = [pltpu.roll(value, LANES - members, axis=1) for value in values]
        down = [pltpu.roll(value, ROWS - 1, axis=0) for value in turned]
        carried = [jnp.where(row == ROWS - 1, down[(half + 1) % halves], down[half]) for half in range(halves)]
        return [jnp.where(lane >= LANES - members, carry, value) for carry, value in zip(carried, turned, strict=True)]

    def previous_run(values):
        turned = [pltpu.roll(value, members, axis=1) for value in values]
        up = [pltpu.roll(value, 1, axis=0) for value in turned]
        carried = [jnp.where(row == 0, up[half - 1], up[half]) for half in range(halves)]
        return [jnp.where(lane < members, carry, value) for carry, value in zip(carried, turned, strict=True)]

    def advance(left_two, left, current, right):
        return [
            (c * (1.0 - TIME_STEP) + FORCING * TIME_STEP * TIME_STEP) + (d - a) * b
            for a, b, c, d in zip(left_two, left, current, right, strict=True)
        ]

    def store(cell, values):
        for half in range(halves):
            begin = cell * tiles + half * ROWS
            state_ref[begin : begin + ROWS, :] = values[half]

    def substep(_, carry):
        before_two = previous_run(group(LANES - 2))
        before = previous_run(group(LANES - 1))
        first = [group(cell) for cell in range(3)]
        beyond = next_run(first[0])
        window = list(first)
        for cell in range(2, LANES - 1):
            right = group(cell + 1)
            store(cell, advance(*window, right))
            window = window[1:] + [right]
        store(LANES - 1, advance(*window, beyond))
        store(0, advance(before_two, before, first[0], first[1]))
        store(1, advance(before, first[0], first[1], first[2]))
        return carry

    lax.fori_loop(0, PREDICT_SUBTICKS, substep, 0)

    for cell in range(LANES):
        for half in range(halves):
            begin = cell * cell_pitch + half * ROWS
            tile_ref[begin : begin + ROWS, :] = group(cell)[half]
    for tile in range(tiles):
        rows_ref[tile_rows(tile), :] = tile_ref[pl.ds(tile, LANES, stride=cell_pitch), :].T * (1.0 / TIME_STEP)
    out_copy = pltpu.make_async_copy(rows_ref, out_ref, out_sem)
    out_copy.start()
    table_copy.wait()

    def gather(block, carry):
        picked = [jnp.zeros((ROWS, LANES), jnp.float32) for _ in range(4)]
        for number in range(LANES):
            begin = pl.multiple_of(scalar_ref[block, number], ROWS)
            turned = pltpu.roll(rows_ref[pl.ds(begin, ROWS), :], scalar_ref[blocks + block, number], axis=1)
            picked[number % 4] = jnp.where(lane == number, turned, picked[number % 4])
        both = picked[0]
        for number in range(1, 4):
            both = jnp.where(lane % 4 == number, picked[number], both)
        part_of = (places_ref[pl.ds(block, 1), :] // LANES) % parts
        chosen = both
        for part in range(1, parts):
            chosen = jnp.where(part_of == part, pltpu.roll(both, ROWS - part * members, axis=0), chosen)
        mine_ref[pl.ds(block * members, members), :] = chosen[:members]
        return carry

    lax.fori_loop(0, blocks, gather, 0)
    for block in range(blocks):
        begin = (blocks + block) * members
        mine_ref[begin : begin + members, :] = noise_ref[:, block * LANES : (block + 1) * LANES]
    out_copy.wait()


def dot(a, b, contract, precision=HIGH):
    return lax.dot_general(a, b, (contract, ((), ())), precision=precision, preferred_element_type=jnp.float32)


def split_three(value):
    high = value.astype(jnp.bfloat16)
    rest = value - high.astype(jnp.float32)
    middle = rest.astype(jnp.bfloat16)
    return high, middle, (rest - middle.astype(jnp.float32)).astype(jnp.bfloat16)


def invert_all(matrix_refs, left_refs, right_refs, done_refs):
    regions = len(matrix_refs)
    size = matrix_refs[0].shape[0]
    panels = size // ROWS
    lane = lanes_iota()
    row = rows_iota()

    def inside(number):
        offset = lane - number * ROWS
        return (offset >= 0) & (offset < ROWS)

    def rows_of(number):
        return pl.ds(pl.multiple_of(number * ROWS, ROWS), ROWS)

    def add_products(group, number):
        for region in group:
            update = dot(left_refs[region][...], right_refs[region][...], ((0,), (0,)), lax.Precision.DEFAULT)
            for i in range(panels):
                rows = slice(i * ROWS, (i + 1) * ROWS)
                matrix_refs[region][rows, :] = jnp.where(inside(number), 0.0, matrix_refs[region][rows, :]) + update[rows]
            matrix_refs[region][rows_of(number), :] = done_refs[region][...]

    def eliminate(group, number):
        offset = lane - number * ROWS
        here = inside(number)
        unit = jnp.where(offset == row, 1.0, 0.0)
        blocks = {region: matrix_refs[region][rows_of(number), :] for region in group}
        columns = []
        for k in range(ROWS):
            index = jnp.full((ROWS, LANES), number * ROWS + k, jnp.int32)
            columns.append({region: jnp.take_along_axis(blocks[region], index, axis=1) for region in group})
        for region in group:
            high, middle, low = split_three(jnp.where(here, 0.0, jnp.where(offset < 0, blocks[region], -blocks[region])))
            left_refs[region][...] = jnp.concatenate([high, high, middle, high, low, middle], axis=0)
            blocks[region] = jnp.where(here, unit, blocks[region])
        for j in range(ROWS):
            at = row == j
            for region in group:
                pivot = columns[j][region]
                inverse = 1.0 / pivot[j : j + 1, :]
                scaled = blocks[region][j : j + 1, :] * inverse
                blocks[region] = jnp.where(at, scaled, blocks[region] - pivot * scaled)
                for k in range(j + 1, ROWS):
                    scaled = columns[k][region][j : j + 1, :] * inverse
                    columns[k][region] = jnp.where(at, scaled, columns[k][region] - pivot * scaled)
        for region in group:
            done_refs[region][...] = blocks[region]
            high, middle, low = split_three(blocks[region])
            right_refs[region][...] = jnp.concatenate([high, middle, high, low, high, middle], axis=0)

    def panel(number, carry):
        eliminate(range(regions), number)
        add_products(range(regions), number)
        return carry

    lax.fori_loop(0, panels, panel, 0)


def invert_scratch(regions, size):
    factor = pltpu.VMEM((6 * ROWS, size), jnp.bfloat16)
    return [[pltpu.VMEM((size, size), jnp.float32)] * regions, [factor] * regions, [factor] * regions, [pltpu.VMEM((ROWS, size), jnp.float32)] * regions]


def split_two(value):
    high = value.astype(jnp.bfloat16)
    return high, (value - high.astype(jnp.float32)).astype(jnp.bfloat16)


def dot_split(a, b, contract):
    a_high, a_low = split_two(a)
    b_high, b_low = split_two(b)
    low = dot(a_high, b_low, contract, lax.Precision.DEFAULT) + dot(a_low, b_high, contract, lax.Precision.DEFAULT)
    return dot(a_high, b_high, contract, lax.Precision.DEFAULT) + low


def prepare_kernel(zone_ref, neighbours_ref, variance_ref, places_ref, pick_ref, errors_ref, *, cells, zone_cells):
    regions, observations, size = pick_ref.shape
    ids = lax.broadcasted_iota(jnp.int32, (observations, size), 0)
    rows = jnp.concatenate([variance_ref[...], places_ref[...].astype(jnp.float32), jnp.zeros((ROWS - 2, observations), jnp.float32)])
    pieces = jnp.concatenate(split_three(rows))
    for region in range(regions):
        zone = zone_ref[0] + region
        pick = jnp.where(ids == neighbours_ref[pl.ds(zone, 1), :], 1.0, 0.0).astype(jnp.bfloat16)
        pick_ref[region, :, :] = pick
        picked = dot(pieces, pick, ((1,), (0,)), lax.Precision.DEFAULT)
        picked = picked[:ROWS] + picked[ROWS : 2 * ROWS] + picked[2 * ROWS :]
        centre = (zone * zone_cells + zone_cells // 2).astype(jnp.float32)
        gap = jnp.abs(picked[1:2] - centre)
        scaled = jnp.minimum(gap, cells - gap) / float(LSCALE)
        errors_ref[region : region + 1, :] = picked[0:1] * (1.0 + scaled * scaled)


def solve_kernel(me_ref, pick_ref, errors_ref, values_ref, variance_ref, *refs, masks):
    *blocks_refs, transform_ref, stack_ref, pieces_ref, matrix_refs, left_refs, right_refs, done_refs = refs
    regions, total, _ = transform_ref.shape
    observations = values_ref.shape[1]
    blocks = observations // LANES
    members = blocks_refs[0].shape[1] // (2 * blocks)
    size = pick_ref.shape[2]
    for block in range(blocks):
        lanes = slice(block * LANES, (block + 1) * LANES)
        values = values_ref[:, lanes]
        spread = jnp.sqrt(variance_ref[:, lanes])
        for blocks_ref, mask in zip(blocks_refs, masks, strict=True):
            for number, bits in enumerate(mask):
                source = pl.multiple_of(lax.bitwise_xor(me_ref[0], bits) * members, members)
                equivalents = blocks_ref[number, block * members : (block + 1) * members, :]
                noise = blocks_ref[number, (blocks + block) * members : (blocks + block + 1) * members, :]
                stack_ref[block, pl.ds(source, members), :] = equivalents
                stack_ref[block, pl.ds(total + source, members), :] = values + spread * noise - equivalents
        for number, piece in enumerate(split_two(stack_ref[block])):
            pieces_ref[number * 2 * total : (number + 1) * 2 * total, lanes] = piece
    diagonal = lax.broadcasted_iota(jnp.int32, (size, size), 0) == lax.broadcasted_iota(jnp.int32, (size, size), 1)
    anomalies, innovations = [], []
    for region in range(regions):
        picked = dot(pieces_ref[...], pick_ref[region], ((1,), (0,)), lax.Precision.DEFAULT)
        picked = picked[: 2 * total] + picked[2 * total :]
        equivalents = picked[:total]
        innovations.append(picked[total:])
        anomaly = equivalents - jnp.sum(equivalents, axis=0, keepdims=True) * (1.0 / total)
        anomalies.append(anomaly)
        high, middle, low = split_three(anomaly.T)
        left = jnp.concatenate([high, high, middle, high, low, middle], axis=1)
        high, middle, low = split_three(anomaly)
        right = jnp.concatenate([high, middle, high, low, high, middle], axis=0)
        covariance = dot(left, right, ((1,), (0,)), lax.Precision.DEFAULT) * (1.0 / (total - 1))
        matrix_refs[region][...] = jnp.where(diagonal, covariance + errors_ref[region : region + 1, :], covariance)
    invert_all(matrix_refs, left_refs, right_refs, done_refs)
    for region in range(regions):
        weights = dot_split(innovations[region], matrix_refs[region][...], ((1,), (0,)))
        transform_ref[region, :, :] = dot_split(weights, anomalies[region], ((1,), (1,))) * (1.0 / (total - 1))


def apply_kernel(counts_ref, transform_ref, cells_ref, owned_ref, block_ref, result_ref, staging_ref, out_sem):
    sources, height, _ = cells_ref.shape
    regions, total, _ = transform_ref.shape
    members = total // sources
    tiles = height // members
    for tile in range(tiles):
        lanes = slice(tile * LANES, (tile + 1) * LANES)
        for source in range(sources):
            block_ref[source * members : (source + 1) * members, lanes] = cells_ref[source, tile * members : (tile + 1) * members, :]
    wide = tiles // regions
    for region in range(regions):
        block = block_ref[:, region * wide * LANES : (region + 1) * wide * LANES]
        anomalies = block - jnp.sum(block, axis=0, keepdims=True) * (1.0 / total)
        analysed = block + dot_split(transform_ref[region], anomalies, ((1,), (0,)))
        for place in range(wide):
            result_ref[region * wide + place, :total, :] = analysed[:, place * LANES : (place + 1) * LANES]
    for tile in range(tiles):
        result_ref[tile, total:, :] = jnp.zeros((ROWS, LANES), jnp.float32)

    def window(destination, offset):
        for tile in range(tiles):
            staging_ref[destination, tile * ROWS : (tile + 1) * ROWS, :] = result_ref[tile, pl.ds(offset, CAP), :]
        return offset + counts_ref[destination]

    groups = out_sem.shape[0]
    group = sources // groups
    offset = jnp.int32(0)
    copies = []
    for number in range(groups):
        offset = lax.fori_loop(number * group, (number + 1) * group, window, offset)
        span = slice(number * group, (number + 1) * group)
        copies.append(pltpu.make_async_copy(staging_ref.at[span], owned_ref.at[span], out_sem.at[number]))
        copies[-1].start()
    for copy in copies:
        copy.wait()


def advance_kernel(count_ref, rows_ref, out_ref, staging_ref, out_sem):
    sources, height, _ = rows_ref.shape
    tiles = height // ROWS
    chunks = out_sem.shape[0]
    here = sources // chunks
    width = here * tiles * LANES
    lane = lanes_iota()
    occupied = rows_iota() < count_ref[0]

    def load(source, tile):
        return rows_ref[source, tile * ROWS : (tile + 1) * ROWS, :]

    def out_copy(chunk):
        lanes = pl.ds(pl.multiple_of(chunk * width, width), width)
        return pltpu.make_async_copy(staging_ref.at[chunk], out_ref.at[:, lanes], out_sem.at[chunk])

    def step(chunk, carry):
        start = chunk * here
        before = load(lax.rem(start + sources - 1, sources), tiles - 1)
        before_one = pltpu.roll(before, 1, axis=1)
        before_two = pltpu.roll(before, 2, axis=1)
        current = load(start, 0)
        current_up = pltpu.roll(current, LANES - 1, axis=1)
        for number in range(here * tiles):
            source, tile = divmod(number + 1, tiles)
            after = load(start + source if source < here else lax.rem(start + here, sources), tile)
            after_up = pltpu.roll(after, LANES - 1, axis=1)
            one = pltpu.roll(current, 1, axis=1)
            two = pltpu.roll(current, 2, axis=1)
            left = jnp.where(lane == 0, before_one, one)
            left_two = jnp.where(lane < 2, before_two, two)
            right = jnp.where(lane == LANES - 1, after_up, current_up)
            stepped = current + TIME_STEP * ((right - left_two) * left - current + FORCING)
            staging_ref[chunk, :, number * LANES : (number + 1) * LANES] = jnp.where(occupied, stepped, 0.0)
            before_one, before_two = one, two
            current, current_up = after, after_up
        out_copy(chunk).start()
        return carry

    lax.fori_loop(0, chunks, step, 0)
    for chunk in range(chunks):
        out_copy(chunk).wait()


def whole(space=pltpu.VMEM):
    return pl.BlockSpec(memory_space=space)


def in_vmem(value):
    return pltpu.with_memory_space_constraint(value, pltpu.VMEM)


def per_device(prior_sample_matrix, obs_values, obs_var, measured_indexes, neighbours, perturbation, counts):
    devices = lax.axis_size(AXES)
    depth = lax.axis_size("region")
    device_index = lax.axis_index(AXES)
    me = device_index.reshape(1)
    members, cells = prior_sample_matrix.shape
    total = members * devices
    observations = obs_values.shape[0]
    zones, local = neighbours.shape
    regions = zones // devices
    zone_cells = cells // zones
    blocks = observations // LANES
    share_tiles = cells // devices // LANES
    values = obs_values.reshape(1, observations)
    variance = obs_var.reshape(1, observations)

    def swap(value, bits):
        return lax.ppermute(value, AXES, [(device, device ^ bits) for device in range(devices)])

    exchange = functools.partial(lax.all_to_all, axis_name=AXES, split_axis=0, concat_axis=0, tiled=True)

    pick, errors = pl.pallas_call(
        functools.partial(prepare_kernel, cells=float(cells), zone_cells=zone_cells),
        out_shape=(pltpu.VMEM((regions, observations, local), jnp.bfloat16), pltpu.VMEM((regions, local), jnp.float32)),
        in_specs=[whole(pltpu.SMEM), whole(), whole(), whole()],
        out_specs=(whole(),) * 2,
        name="prepare",
    )(me * regions, neighbours, variance, measured_indexes.reshape(1, observations))

    runs = prior_sample_matrix.reshape(members, cells // LANES, LANES).transpose(1, 0, 2).reshape(-1, LANES)
    height = runs.shape[0]
    tiles = height // LANES
    state, mine = pl.pallas_call(
        functools.partial(forecast_kernel, members=members),
        out_shape=(
            jax.ShapeDtypeStruct((height, LANES), jnp.float32),
            jax.ShapeDtypeStruct((2 * blocks * members, LANES), jnp.float32),
        ),
        in_specs=[whole()] * 3,
        out_specs=(whole(pltpu.HBM), whole()),
        scratch_shapes=[
            pltpu.VMEM((height, LANES), jnp.float32),
            pltpu.VMEM((height, LANES), jnp.float32),
            pltpu.VMEM((max(tiles * (LANES + ROWS), LANES * (tiles + ROWS)), LANES), jnp.float32),
            pltpu.VMEM((2 * blocks, LANES), jnp.int32),
            pltpu.SMEM((2 * blocks, LANES), jnp.int32),
            pltpu.SemaphoreType.DMA,
            pltpu.SemaphoreType.DMA,
        ],
        name="forecast",
    )(measured_indexes.reshape(blocks, LANES), perturbation, runs)

    near = jnp.concatenate([mine[None]] + [swap(mine[None], bits) for bits in range(1, depth)])
    near_mask = list(range(depth))
    far_masks = [[chip * 2 * depth + bits for bits in near_mask] for chip in range(1, devices // (2 * depth))]
    far = []
    for mask in far_masks:
        far.append(swap(near, mask[0]))
    own_cells = exchange(state.reshape(devices, height // devices, LANES))
    partner = swap(near, depth)
    partners = swap(jnp.concatenate(far), depth)
    pieces = [near, partner, *far, partners]
    masks = [near_mask, [depth ^ bits for bits in near_mask], *far_masks, [depth ^ bits for mask in far_masks for bits in mask]]

    place = in_vmem if sum(piece.size for piece in pieces) * 4 <= VMEM_PIECES else lambda value: value
    transform = pl.pallas_call(
        functools.partial(solve_kernel, masks=masks),
        out_shape=pltpu.VMEM((regions, total, total), jnp.float32),
        in_specs=[whole(pltpu.SMEM)] + [whole()] * (4 + len(pieces)),
        out_specs=whole(),
        scratch_shapes=[
            pltpu.VMEM((blocks, 2 * total, LANES), jnp.float32),
            pltpu.VMEM((4 * total, observations), jnp.bfloat16),
            *invert_scratch(regions, local),
        ],
        name="solve",
    )(me, place(pick), place(errors), values, variance, *map(place, pieces))

    outgoing = pl.pallas_call(
        apply_kernel,
        out_shape=jax.ShapeDtypeStruct((devices, share_tiles * CAP, LANES), jnp.float32),
        in_specs=[whole(pltpu.SMEM), whole(), whole()],
        out_specs=whole(pltpu.HBM),
        scratch_shapes=[
            pltpu.VMEM((total, share_tiles * LANES), jnp.float32),
            pltpu.VMEM((share_tiles, total + ROWS, LANES), jnp.float32),
            pltpu.VMEM((devices, share_tiles * CAP, LANES), jnp.float32),
            pltpu.SemaphoreType.DMA((4,)),
        ],
        name="analyse",
    )(counts, in_vmem(transform), in_vmem(own_cells))
    owned = exchange(outgoing)

    chunks = 8
    return pl.pallas_call(
        advance_kernel,
        out_shape=jax.ShapeDtypeStruct((CAP, cells), jnp.float32),
        in_specs=[whole(pltpu.SMEM), whole()],
        out_specs=whole(pltpu.HBM),
        scratch_shapes=[pltpu.VMEM((chunks, CAP, cells // chunks), jnp.float32), pltpu.SemaphoreType.DMA((chunks,))],
        name="advance",
    )(lax.dynamic_slice_in_dim(counts, device_index, 1, 0), in_vmem(owned))


def solution(mesh):
    rows = P(AXES, None)
    return jax.shard_map(
        per_device, mesh=mesh, in_specs=(rows, P(), P(), P(), P(), rows, P()), out_specs=rows, check_vma=False
    )
```

```python
import functools

import jax
import jax.numpy as jnp
from jax import lax
from jax.experimental import pallas as pl
from jax.experimental.pallas import tpu as pltpu
from jax.sharding import PartitionSpec as P


PREDICT_SUBTICKS = 24
CAP = 8
LSCALE = 2048
FORCING = 8.0
TIME_STEP = 0.01
HIGH = lax.Precision.HIGHEST
AXES = ("member", "region")
LANES = 128
VMEM_PIECES = 1 << 20
ROWS = 8


def lanes_iota():
    return lax.broadcasted_iota(jnp.int32, (ROWS, LANES), 1)


def rows_iota():
    return lax.broadcasted_iota(jnp.int32, (ROWS, LANES), 0)


def forecast_kernel(places_ref, noise_ref, x_ref, out_ref, mine_ref, rows_ref, state_ref, tile_ref, table_ref, scalar_ref, table_sem, out_sem, *, members):
    height = x_ref.shape[0]
    blocks = places_ref.shape[0]
    tiles = height // LANES
    halves = tiles // ROWS
    tile_pitch = LANES + ROWS
    cell_pitch = tiles + ROWS
    parts = ROWS // members
    lane = lanes_iota()
    row = rows_iota()

    def group(cell):
        return [state_ref[cell * tiles + half * ROWS : cell * tiles + (half + 1) * ROWS, :] for half in range(halves)]

    def tile_rows(tile):
        return slice(tile * LANES, (tile + 1) * LANES)

    for tile in range(tiles):
        tile_ref[tile * tile_pitch : tile * tile_pitch + LANES, :] = (x_ref[tile_rows(tile), :] * TIME_STEP).T
    for cell in range(LANES):
        for half in range(halves):
            begin = cell * tiles + half * ROWS
            state_ref[begin : begin + ROWS, :] = tile_ref[pl.ds(half * ROWS * tile_pitch + cell, ROWS, stride=tile_pitch), :]

    places = places_ref[...]
    column = lax.broadcasted_iota(jnp.int32, places.shape, 1)
    table_ref[:blocks, :] = (places // (LANES * parts)) * ROWS
    table_ref[blocks:, :] = (column - places) & (LANES - 1)
    table_copy = pltpu.make_async_copy(table_ref, scalar_ref, table_sem)
    table_copy.start()

    def next_run(values):
        turned = [pltpu.roll(value, LANES - members, axis=1) for value in values]
        down = [pltpu.roll(value, ROWS - 1, axis=0) for value in turned]
        carried = [jnp.where(row == ROWS - 1, down[(half + 1) % halves], down[half]) for half in range(halves)]
        return [jnp.where(lane >= LANES - members, carry, value) for carry, value in zip(carried, turned, strict=True)]

    def previous_run(values):
        turned = [pltpu.roll(value, members, axis=1) for value in values]
        up = [pltpu.roll(value, 1, axis=0) for value in turned]
        carried = [jnp.where(row == 0, up[half - 1], up[half]) for half in range(halves)]
        return [jnp.where(lane < members, carry, value) for carry, value in zip(carried, turned, strict=True)]

    def advance(left_two, left, current, right):
        return [
            (c * (1.0 - TIME_STEP) + FORCING * TIME_STEP * TIME_STEP) + (d - a) * b
            for a, b, c, d in zip(left_two, left, current, right, strict=True)
        ]

    def store(cell, values):
        for half in range(halves):
            begin = cell * tiles + half * ROWS
            state_ref[begin : begin + ROWS, :] = values[half]

    def substep(_, carry):
        before_two = previous_run(group(LANES - 2))
        before = previous_run(group(LANES - 1))
        first = [group(cell) for cell in range(3)]
        beyond = next_run(first[0])
        window = list(first)
        for cell in range(2, LANES - 1):
            right = group(cell + 1)
            store(cell, advance(*window, right))
            window = window[1:] + [right]
        store(LANES - 1, advance(*window, beyond))
        store(0, advance(before_two, before, first[0], first[1]))
        store(1, advance(before, first[0], first[1], first[2]))
        return carry

    lax.fori_loop(0, PREDICT_SUBTICKS, substep, 0)

    for cell in range(LANES):
        for half in range(halves):
            begin = cell * cell_pitch + half * ROWS
            tile_ref[begin : begin + ROWS, :] = group(cell)[half]
    for tile in range(tiles):
        rows_ref[tile_rows(tile), :] = tile_ref[pl.ds(tile, LANES, stride=cell_pitch), :].T * (1.0 / TIME_STEP)
    out_copy = pltpu.make_async_copy(rows_ref, out_ref, out_sem)
    out_copy.start()
    table_copy.wait()

    for block in range(blocks):
        picked = [jnp.zeros((ROWS, LANES), jnp.float32) for _ in range(4)]
        for number in range(LANES):
            begin = pl.multiple_of(scalar_ref[block, number], ROWS)
            turned = pltpu.roll(rows_ref[pl.ds(begin, ROWS), :], scalar_ref[blocks + block, number], axis=1)
            picked[number % 4] = jnp.where(lane == number, turned, picked[number % 4])
        both = picked[0]
        for number in range(1, 4):
            both = jnp.where(lane % 4 == number, picked[number], both)
        part_of = (places_ref[block : block + 1, :] // LANES) % parts
        chosen = both
        for part in range(1, parts):
            chosen = jnp.where(part_of == part, pltpu.roll(both, ROWS - part * members, axis=0), chosen)
        mine_ref[block * members : (block + 1) * members, :] = chosen[:members]
    for block in range(blocks):
        begin = (blocks + block) * members
        mine_ref[begin : begin + members, :] = noise_ref[:, block * LANES : (block + 1) * LANES]
    out_copy.wait()


def dot(a, b, contract, precision=HIGH):
    return lax.dot_general(a, b, (contract, ((), ())), precision=precision, preferred_element_type=jnp.float32)


def split_three(value):
    high = value.astype(jnp.bfloat16)
    rest = value - high.astype(jnp.float32)
    middle = rest.astype(jnp.bfloat16)
    return high, middle, (rest - middle.astype(jnp.float32)).astype(jnp.bfloat16)


def invert_all(matrix_refs, left_refs, right_refs, done_refs):
    regions = len(matrix_refs)
    size = matrix_refs[0].shape[0]
    panels = size // ROWS
    lane = lanes_iota()
    row = rows_iota()

    def inside(number):
        offset = lane - number * ROWS
        return (offset >= 0) & (offset < ROWS)

    def rows_of(number):
        return pl.ds(pl.multiple_of(number * ROWS, ROWS), ROWS)

    def add_products(group, number):
        for region in group:
            update = dot(left_refs[region][...], right_refs[region][...], ((0,), (0,)), lax.Precision.DEFAULT)
            for i in range(panels):
                rows = slice(i * ROWS, (i + 1) * ROWS)
                matrix_refs[region][rows, :] = jnp.where(inside(number), 0.0, matrix_refs[region][rows, :]) + update[rows]
            matrix_refs[region][rows_of(number), :] = done_refs[region][...]

    def eliminate(group, number):
        offset = lane - number * ROWS
        here = inside(number)
        unit = jnp.where(offset == row, 1.0, 0.0)
        blocks = {region: matrix_refs[region][rows_of(number), :] for region in group}
        columns = []
        for k in range(ROWS):
            index = jnp.full((ROWS, LANES), number * ROWS + k, jnp.int32)
            columns.append({region: jnp.take_along_axis(blocks[region], index, axis=1) for region in group})
        for region in group:
            high, middle, low = split_three(jnp.where(here, 0.0, jnp.where(offset < 0, blocks[region], -blocks[region])))
            left_refs[region][...] = jnp.concatenate([high, high, middle, high, low, middle], axis=0)
            blocks[region] = jnp.where(here, unit, blocks[region])
        for j in range(ROWS):
            at = row == j
            for region in group:
                pivot = columns[j][region]
                inverse = 1.0 / pivot[j : j + 1, :]
                scaled = blocks[region][j : j + 1, :] * inverse
                blocks[region] = jnp.where(at, scaled, blocks[region] - pivot * scaled)
                for k in range(j + 1, ROWS):
                    scaled = columns[k][region][j : j + 1, :] * inverse
                    columns[k][region] = jnp.where(at, scaled, columns[k][region] - pivot * scaled)
        for region in group:
            done_refs[region][...] = blocks[region]
            high, middle, low = split_three(blocks[region])
            right_refs[region][...] = jnp.concatenate([high, middle, high, low, high, middle], axis=0)

    def panel(number, carry):
        eliminate(range(regions), number)
        add_products(range(regions), number)
        return carry

    lax.fori_loop(0, panels, panel, 0)


def invert_scratch(regions, size):
    factor = pltpu.VMEM((6 * ROWS, size), jnp.bfloat16)
    return [[pltpu.VMEM((size, size), jnp.float32)] * regions, [factor] * regions, [factor] * regions, [pltpu.VMEM((ROWS, size), jnp.float32)] * regions]


def split_two(value):
    high = value.astype(jnp.bfloat16)
    return high, (value - high.astype(jnp.float32)).astype(jnp.bfloat16)


def dot_split(a, b, contract):
    a_high, a_low = split_two(a)
    b_high, b_low = split_two(b)
    low = dot(a_high, b_low, contract, lax.Precision.DEFAULT) + dot(a_low, b_high, contract, lax.Precision.DEFAULT)
    return dot(a_high, b_high, contract, lax.Precision.DEFAULT) + low


def prepare_kernel(zone_ref, neighbours_ref, variance_ref, places_ref, pick_ref, errors_ref, *, cells, zone_cells):
    regions, observations, size = pick_ref.shape
    ids = lax.broadcasted_iota(jnp.int32, (observations, size), 0)
    rows = jnp.concatenate([variance_ref[...], places_ref[...].astype(jnp.float32), jnp.zeros((ROWS - 2, observations), jnp.float32)])
    pieces = jnp.concatenate(split_three(rows))
    for region in range(regions):
        zone = zone_ref[0] + region
        pick = jnp.where(ids == neighbours_ref[pl.ds(zone, 1), :], 1.0, 0.0).astype(jnp.bfloat16)
        pick_ref[region, :, :] = pick
        picked = dot(pieces, pick, ((1,), (0,)), lax.Precision.DEFAULT)
        picked = picked[:ROWS] + picked[ROWS : 2 * ROWS] + picked[2 * ROWS :]
        centre = (zone * zone_cells + zone_cells // 2).astype(jnp.float32)
        gap = jnp.abs(picked[1:2] - centre)
        scaled = jnp.minimum(gap, cells - gap) / float(LSCALE)
        errors_ref[region : region + 1, :] = picked[0:1] * (1.0 + scaled * scaled)


def solve_kernel(me_ref, pick_ref, errors_ref, values_ref, variance_ref, *refs, masks):
    *blocks_refs, transform_ref, stack_ref, pieces_ref, matrix_refs, left_refs, right_refs, done_refs = refs
    regions, total, _ = transform_ref.shape
    observations = values_ref.shape[1]
    blocks = observations // LANES
    members = blocks_refs[0].shape[1] // (2 * blocks)
    size = pick_ref.shape[2]
    for block in range(blocks):
        lanes = slice(block * LANES, (block + 1) * LANES)
        values = values_ref[:, lanes]
        spread = jnp.sqrt(variance_ref[:, lanes])
        for blocks_ref, mask in zip(blocks_refs, masks, strict=True):
            for number, bits in enumerate(mask):
                source = pl.multiple_of(lax.bitwise_xor(me_ref[0], bits) * members, members)
                equivalents = blocks_ref[number, block * members : (block + 1) * members, :]
                noise = blocks_ref[number, (blocks + block) * members : (blocks + block + 1) * members, :]
                stack_ref[block, pl.ds(source, members), :] = equivalents
                stack_ref[block, pl.ds(total + source, members), :] = values + spread * noise - equivalents
        for number, piece in enumerate(split_two(stack_ref[block])):
            pieces_ref[number * 2 * total : (number + 1) * 2 * total, lanes] = piece
    diagonal = lax.broadcasted_iota(jnp.int32, (size, size), 0) == lax.broadcasted_iota(jnp.int32, (size, size), 1)
    anomalies, innovations = [], []
    for region in range(regions):
        picked = dot(pieces_ref[...], pick_ref[region], ((1,), (0,)), lax.Precision.DEFAULT)
        picked = picked[: 2 * total] + picked[2 * total :]
        equivalents = picked[:total]
        innovations.append(picked[total:])
        anomaly = equivalents - jnp.sum(equivalents, axis=0, keepdims=True) * (1.0 / total)
        anomalies.append(anomaly)
        high, middle, low = split_three(anomaly.T)
        left = jnp.concatenate([high, high, middle, high, low, middle], axis=1)
        high, middle, low = split_three(anomaly)
        right = jnp.concatenate([high, middle, high, low, high, middle], axis=0)
        covariance = dot(left, right, ((1,), (0,)), lax.Precision.DEFAULT) * (1.0 / (total - 1))
        matrix_refs[region][...] = jnp.where(diagonal, covariance + errors_ref[region : region + 1, :], covariance)
    invert_all(matrix_refs, left_refs, right_refs, done_refs)
    for region in range(regions):
        weights = dot_split(innovations[region], matrix_refs[region][...], ((1,), (0,)))
        transform_ref[region, :, :] = dot_split(weights, anomalies[region], ((1,), (1,))) * (1.0 / (total - 1))


def apply_kernel(counts_ref, transform_ref, cells_ref, owned_ref, block_ref, result_ref, staging_ref, out_sem):
    sources, height, _ = cells_ref.shape
    regions, total, _ = transform_ref.shape
    members = total // sources
    tiles = height // members
    for tile in range(tiles):
        lanes = slice(tile * LANES, (tile + 1) * LANES)
        for source in range(sources):
            block_ref[source * members : (source + 1) * members, lanes] = cells_ref[source, tile * members : (tile + 1) * members, :]
    wide = tiles // regions
    for region in range(regions):
        block = block_ref[:, region * wide * LANES : (region + 1) * wide * LANES]
        anomalies = block - jnp.sum(block, axis=0, keepdims=True) * (1.0 / total)
        analysed = block + dot_split(transform_ref[region], anomalies, ((1,), (0,)))
        for place in range(wide):
            result_ref[region * wide + place, :total, :] = analysed[:, place * LANES : (place + 1) * LANES]
    for tile in range(tiles):
        result_ref[tile, total:, :] = jnp.zeros((ROWS, LANES), jnp.float32)

    def window(destination, offset):
        for tile in range(tiles):
            staging_ref[destination, tile * ROWS : (tile + 1) * ROWS, :] = result_ref[tile, pl.ds(offset, CAP), :]
        return offset + counts_ref[destination]

    groups = out_sem.shape[0]
    group = sources // groups
    offset = jnp.int32(0)
    copies = []
    for number in range(groups):
        offset = lax.fori_loop(number * group, (number + 1) * group, window, offset, unroll=True)
        span = slice(number * group, (number + 1) * group)
        copies.append(pltpu.make_async_copy(staging_ref.at[span], owned_ref.at[span], out_sem.at[number]))
        copies[-1].start()
    for copy in copies:
        copy.wait()


def advance_kernel(count_ref, rows_ref, out_ref, staging_ref, out_sem):
    sources, height, _ = rows_ref.shape
    tiles = height // ROWS
    chunks = out_sem.shape[0]
    here = sources // chunks
    width = here * tiles * LANES
    lane = lanes_iota()
    occupied = rows_iota() < count_ref[0]

    def load(source, tile):
        return rows_ref[source, tile * ROWS : (tile + 1) * ROWS, :]

    def out_copy(chunk):
        lanes = pl.ds(pl.multiple_of(chunk * width, width), width)
        return pltpu.make_async_copy(staging_ref.at[chunk], out_ref.at[:, lanes], out_sem.at[chunk])

    def step(chunk, carry):
        start = chunk * here
        before = load(lax.rem(start + sources - 1, sources), tiles - 1)
        before_one = pltpu.roll(before, 1, axis=1)
        before_two = pltpu.roll(before, 2, axis=1)
        current = load(start, 0)
        current_up = pltpu.roll(current, LANES - 1, axis=1)
        for number in range(here * tiles):
            source, tile = divmod(number + 1, tiles)
            after = load(start + source if source < here else lax.rem(start + here, sources), tile)
            after_up = pltpu.roll(after, LANES - 1, axis=1)
            one = pltpu.roll(current, 1, axis=1)
            two = pltpu.roll(current, 2, axis=1)
            left = jnp.where(lane == 0, before_one, one)
            left_two = jnp.where(lane < 2, before_two, two)
            right = jnp.where(lane == LANES - 1, after_up, current_up)
            stepped = current + TIME_STEP * ((right - left_two) * left - current + FORCING)
            staging_ref[chunk, :, number * LANES : (number + 1) * LANES] = jnp.where(occupied, stepped, 0.0)
            before_one, before_two = one, two
            current, current_up = after, after_up
        out_copy(chunk).start()
        return carry

    lax.fori_loop(0, chunks, step, 0)
    for chunk in range(chunks):
        out_copy(chunk).wait()


def whole(space=pltpu.VMEM):
    return pl.BlockSpec(memory_space=space)


def in_vmem(value):
    return pltpu.with_memory_space_constraint(value, pltpu.VMEM)


def per_device(prior_sample_matrix, obs_values, obs_var, measured_indexes, neighbours, perturbation, counts):
    devices = lax.axis_size(AXES)
    depth = lax.axis_size("region")
    device_index = lax.axis_index(AXES)
    me = device_index.reshape(1)
    members, cells = prior_sample_matrix.shape
    total = members * devices
    observations = obs_values.shape[0]
    zones, local = neighbours.shape
    regions = zones // devices
    zone_cells = cells // zones
    blocks = observations // LANES
    share_tiles = cells // devices // LANES
    values = obs_values.reshape(1, observations)
    variance = obs_var.reshape(1, observations)

    def swap(value, bits):
        return lax.ppermute(value, AXES, [(device, device ^ bits) for device in range(devices)])

    exchange = functools.partial(lax.all_to_all, axis_name=AXES, split_axis=0, concat_axis=0, tiled=True)

    pick, errors = pl.pallas_call(
        functools.partial(prepare_kernel, cells=float(cells), zone_cells=zone_cells),
        out_shape=(pltpu.VMEM((regions, observations, local), jnp.bfloat16), pltpu.VMEM((regions, local), jnp.float32)),
        in_specs=[whole(pltpu.SMEM), whole(), whole(), whole()],
        out_specs=(whole(),) * 2,
        name="prepare",
    )(me * regions, neighbours, variance, measured_indexes.reshape(1, observations))

    runs = prior_sample_matrix.reshape(members, cells // LANES, LANES).transpose(1, 0, 2).reshape(-1, LANES)
    height = runs.shape[0]
    tiles = height // LANES
    state, mine = pl.pallas_call(
        functools.partial(forecast_kernel, members=members),
        out_shape=(
            jax.ShapeDtypeStruct((height, LANES), jnp.float32),
            jax.ShapeDtypeStruct((2 * blocks * members, LANES), jnp.float32),
        ),
        in_specs=[whole()] * 3,
        out_specs=(whole(pltpu.HBM), whole()),
        scratch_shapes=[
            pltpu.VMEM((height, LANES), jnp.float32),
            pltpu.VMEM((height, LANES), jnp.float32),
            pltpu.VMEM((max(tiles * (LANES + ROWS), LANES * (tiles + ROWS)), LANES), jnp.float32),
            pltpu.VMEM((2 * blocks, LANES), jnp.int32),
            pltpu.SMEM((2 * blocks, LANES), jnp.int32),
            pltpu.SemaphoreType.DMA,
            pltpu.SemaphoreType.DMA,
        ],
        name="forecast",
    )(measured_indexes.reshape(blocks, LANES), perturbation, runs)

    near = jnp.concatenate([mine[None]] + [swap(mine[None], bits) for bits in range(1, depth)])
    near_mask = list(range(depth))
    far_masks = [[chip * 2 * depth + bits for bits in near_mask] for chip in range(1, devices // (2 * depth))]
    far = []
    for mask in far_masks:
        far.append(swap(near, mask[0]))
    own_cells = exchange(state.reshape(devices, height // devices, LANES))
    partner = swap(near, depth)
    partners = swap(jnp.concatenate(far), depth)
    pieces = [near, partner, *far, partners]
    masks = [near_mask, [depth ^ bits for bits in near_mask], *far_masks, [depth ^ bits for mask in far_masks for bits in mask]]

    place = in_vmem if sum(piece.size for piece in pieces) * 4 <= VMEM_PIECES else lambda value: value
    transform = pl.pallas_call(
        functools.partial(solve_kernel, masks=masks),
        out_shape=pltpu.VMEM((regions, total, total), jnp.float32),
        in_specs=[whole(pltpu.SMEM)] + [whole()] * (4 + len(pieces)),
        out_specs=whole(),
        scratch_shapes=[
            pltpu.VMEM((blocks, 2 * total, LANES), jnp.float32),
            pltpu.VMEM((4 * total, observations), jnp.bfloat16),
            *invert_scratch(regions, local),
        ],
        name="solve",
    )(me, place(pick), place(errors), values, variance, *map(place, pieces))

    outgoing = pl.pallas_call(
        apply_kernel,
        out_shape=jax.ShapeDtypeStruct((devices, share_tiles * CAP, LANES), jnp.float32),
        in_specs=[whole(pltpu.SMEM), whole(), whole()],
        out_specs=whole(pltpu.HBM),
        scratch_shapes=[
            pltpu.VMEM((total, share_tiles * LANES), jnp.float32),
            pltpu.VMEM((share_tiles, total + ROWS, LANES), jnp.float32),
            pltpu.VMEM((devices, share_tiles * CAP, LANES), jnp.float32),
            pltpu.SemaphoreType.DMA((4,)),
        ],
        name="analyse",
    )(counts, in_vmem(transform), in_vmem(own_cells))
    owned = exchange(outgoing)

    chunks = 4
    return pl.pallas_call(
        advance_kernel,
        out_shape=jax.ShapeDtypeStruct((CAP, cells), jnp.float32),
        in_specs=[whole(pltpu.SMEM), whole()],
        out_specs=whole(pltpu.HBM),
        scratch_shapes=[pltpu.VMEM((chunks, CAP, cells // chunks), jnp.float32), pltpu.SemaphoreType.DMA((chunks,))],
        name="advance",
    )(lax.dynamic_slice_in_dim(counts, device_index, 1, 0), in_vmem(owned))


def solution(mesh):
    rows = P(AXES, None)
    return jax.shard_map(
        per_device, mesh=mesh, in_specs=(rows, P(), P(), P(), P(), rows, P()), out_specs=rows, check_vma=False
    )
```

```python
import functools

import jax
import jax.numpy as jnp
from jax import lax
from jax.experimental import pallas as pl
from jax.experimental.pallas import tpu as pltpu
from jax.sharding import PartitionSpec as P


PREDICT_SUBTICKS = 24
CAP = 8
LSCALE = 2048
FORCING = 8.0
TIME_STEP = 0.01
HIGH = lax.Precision.HIGHEST
AXES = ("member", "region")
LANES = 128
VMEM_PIECES = 1 << 20
ROWS = 8


def lanes_iota():
    return lax.broadcasted_iota(jnp.int32, (ROWS, LANES), 1)


def rows_iota():
    return lax.broadcasted_iota(jnp.int32, (ROWS, LANES), 0)


def forecast_kernel(places_ref, noise_ref, x_ref, out_ref, mine_ref, rows_ref, state_ref, tile_ref, table_ref, scalar_ref, table_sem, out_sem, *, members):
    height = x_ref.shape[0]
    blocks = places_ref.shape[0]
    tiles = height // LANES
    halves = tiles // ROWS
    tile_pitch = LANES + ROWS
    cell_pitch = tiles + ROWS
    parts = ROWS // members
    lane = lanes_iota()
    row = rows_iota()

    def group(cell):
        return [state_ref[cell * tiles + half * ROWS : cell * tiles + (half + 1) * ROWS, :] for half in range(halves)]

    def tile_rows(tile):
        return slice(tile * LANES, (tile + 1) * LANES)

    for tile in range(tiles):
        tile_ref[tile * tile_pitch : tile * tile_pitch + LANES, :] = (x_ref[tile_rows(tile), :] * TIME_STEP).T
    for cell in range(LANES):
        for half in range(halves):
            begin = cell * tiles + half * ROWS
            state_ref[begin : begin + ROWS, :] = tile_ref[pl.ds(half * ROWS * tile_pitch + cell, ROWS, stride=tile_pitch), :]

    places = places_ref[...]
    column = lax.broadcasted_iota(jnp.int32, places.shape, 1)
    table_ref[:blocks, :] = (places // (LANES * parts)) * ROWS
    table_ref[blocks:, :] = (column - places) & (LANES - 1)
    table_copy = pltpu.make_async_copy(table_ref, scalar_ref, table_sem)
    table_copy.start()

    def next_run(values):
        turned = [pltpu.roll(value, LANES - members, axis=1) for value in values]
        down = [pltpu.roll(value, ROWS - 1, axis=0) for value in turned]
        carried = [jnp.where(row == ROWS - 1, down[(half + 1) % halves], down[half]) for half in range(halves)]
        return [jnp.where(lane >= LANES - members, carry, value) for carry, value in zip(carried, turned, strict=True)]

    def previous_run(values):
        turned = [pltpu.roll(value, members, axis=1) for value in values]
        up = [pltpu.roll(value, 1, axis=0) for value in turned]
        carried = [jnp.where(row == 0, up[half - 1], up[half]) for half in range(halves)]
        return [jnp.where(lane < members, carry, value) for carry, value in zip(carried, turned, strict=True)]

    def advance(left_two, left, current, right):
        return [
            (c * (1.0 - TIME_STEP) + FORCING * TIME_STEP * TIME_STEP) + (d - a) * b
            for a, b, c, d in zip(left_two, left, current, right, strict=True)
        ]

    def store(cell, values):
        for half in range(halves):
            begin = cell * tiles + half * ROWS
            state_ref[begin : begin + ROWS, :] = values[half]

    def substep(_, carry):
        before_two = previous_run(group(LANES - 2))
        before = previous_run(group(LANES - 1))
        first = [group(cell) for cell in range(3)]
        beyond = next_run(first[0])
        window = list(first)
        for cell in range(2, LANES - 1):
            right = group(cell + 1)
            store(cell, advance(*window, right))
            window = window[1:] + [right]
        store(LANES - 1, advance(*window, beyond))
        store(0, advance(before_two, before, first[0], first[1]))
        store(1, advance(before, first[0], first[1], first[2]))
        return carry

    lax.fori_loop(0, PREDICT_SUBTICKS, substep, 0)

    for cell in range(LANES):
        for half in range(halves):
            begin = cell * cell_pitch + half * ROWS
            tile_ref[begin : begin + ROWS, :] = group(cell)[half]
    for tile in range(tiles):
        rows_ref[tile_rows(tile), :] = tile_ref[pl.ds(tile, LANES, stride=cell_pitch), :].T * (1.0 / TIME_STEP)
    out_copy = pltpu.make_async_copy(rows_ref, out_ref, out_sem)
    out_copy.start()
    table_copy.wait()

    for block in range(blocks):
        picked = [jnp.zeros((ROWS, LANES), jnp.float32) for _ in range(4)]
        for number in range(LANES):
            begin = pl.multiple_of(scalar_ref[block, number], ROWS)
            turned = pltpu.roll(rows_ref[pl.ds(begin, ROWS), :], scalar_ref[blocks + block, number], axis=1)
            picked[number % 4] = jnp.where(lane == number, turned, picked[number % 4])
        both = picked[0]
        for number in range(1, 4):
            both = jnp.where(lane % 4 == number, picked[number], both)
        part_of = (places_ref[block : block + 1, :] // LANES) % parts
        chosen = both
        for part in range(1, parts):
            chosen = jnp.where(part_of == part, pltpu.roll(both, ROWS - part * members, axis=0), chosen)
        mine_ref[block * members : (block + 1) * members, :] = chosen[:members]
    for block in range(blocks):
        begin = (blocks + block) * members
        mine_ref[begin : begin + members, :] = noise_ref[:, block * LANES : (block + 1) * LANES]
    out_copy.wait()


def dot(a, b, contract, precision=HIGH):
    return lax.dot_general(a, b, (contract, ((), ())), precision=precision, preferred_element_type=jnp.float32)


def split_three(value):
    high = value.astype(jnp.bfloat16)
    rest = value - high.astype(jnp.float32)
    middle = rest.astype(jnp.bfloat16)
    return high, middle, (rest - middle.astype(jnp.float32)).astype(jnp.bfloat16)


def invert_all(matrix_refs, left_refs, right_refs, done_refs):
    regions = len(matrix_refs)
    size = matrix_refs[0].shape[0]
    panels = size // ROWS
    lane = lanes_iota()
    row = rows_iota()

    def inside(number):
        offset = lane - number * ROWS
        return (offset >= 0) & (offset < ROWS)

    def rows_of(number):
        return pl.ds(pl.multiple_of(number * ROWS, ROWS), ROWS)

    def add_products(group, number):
        for region in group:
            update = dot(left_refs[region][...], right_refs[region][...], ((0,), (0,)), lax.Precision.DEFAULT)
            for i in range(panels):
                rows = slice(i * ROWS, (i + 1) * ROWS)
                matrix_refs[region][rows, :] = jnp.where(inside(number), 0.0, matrix_refs[region][rows, :]) + update[rows]
            matrix_refs[region][rows_of(number), :] = done_refs[region][...]

    def eliminate(group, number):
        offset = lane - number * ROWS
        here = inside(number)
        unit = jnp.where(offset == row, 1.0, 0.0)
        blocks = {region: matrix_refs[region][rows_of(number), :] for region in group}
        columns = []
        for k in range(ROWS):
            index = jnp.full((ROWS, LANES), number * ROWS + k, jnp.int32)
            columns.append({region: jnp.take_along_axis(blocks[region], index, axis=1) for region in group})
        for region in group:
            high, middle, low = split_three(jnp.where(here, 0.0, jnp.where(offset < 0, blocks[region], -blocks[region])))
            left_refs[region][...] = jnp.concatenate([high, high, middle, high, low, middle], axis=0)
            blocks[region] = jnp.where(here, unit, blocks[region])
        for j in range(ROWS):
            at = row == j
            for region in group:
                pivot = columns[j][region]
                inverse = 1.0 / pivot[j : j + 1, :]
                scaled = blocks[region][j : j + 1, :] * inverse
                blocks[region] = jnp.where(at, scaled, blocks[region] - pivot * scaled)
                for k in range(j + 1, ROWS):
                    scaled = columns[k][region][j : j + 1, :] * inverse
                    columns[k][region] = jnp.where(at, scaled, columns[k][region] - pivot * scaled)
        for region in group:
            done_refs[region][...] = blocks[region]
            high, middle, low = split_three(blocks[region])
            right_refs[region][...] = jnp.concatenate([high, middle, high, low, high, middle], axis=0)

    def panel(number, carry):
        eliminate(range(regions), number)
        add_products(range(regions), number)
        return carry

    lax.fori_loop(0, panels, panel, 0)


def invert_scratch(regions, size):
    factor = pltpu.VMEM((6 * ROWS, size), jnp.bfloat16)
    return [[pltpu.VMEM((size, size), jnp.float32)] * regions, [factor] * regions, [factor] * regions, [pltpu.VMEM((ROWS, size), jnp.float32)] * regions]


def split_two(value):
    high = value.astype(jnp.bfloat16)
    return high, (value - high.astype(jnp.float32)).astype(jnp.bfloat16)


def dot_split(a, b, contract):
    a_high, a_low = split_two(a)
    b_high, b_low = split_two(b)
    low = dot(a_high, b_low, contract, lax.Precision.DEFAULT) + dot(a_low, b_high, contract, lax.Precision.DEFAULT)
    return dot(a_high, b_high, contract, lax.Precision.DEFAULT) + low


def prepare_kernel(zone_ref, neighbours_ref, variance_ref, places_ref, pick_ref, errors_ref, *, cells, zone_cells):
    regions, observations, size = pick_ref.shape
    ids = lax.broadcasted_iota(jnp.int32, (observations, size), 0)
    rows = jnp.concatenate([variance_ref[...], places_ref[...].astype(jnp.float32), jnp.zeros((ROWS - 2, observations), jnp.float32)])
    pieces = jnp.concatenate(split_three(rows))
    for region in range(regions):
        zone = zone_ref[0] + region
        pick = jnp.where(ids == neighbours_ref[pl.ds(zone, 1), :], 1.0, 0.0).astype(jnp.bfloat16)
        pick_ref[region, :, :] = pick
        picked = dot(pieces, pick, ((1,), (0,)), lax.Precision.DEFAULT)
        picked = picked[:ROWS] + picked[ROWS : 2 * ROWS] + picked[2 * ROWS :]
        centre = (zone * zone_cells + zone_cells // 2).astype(jnp.float32)
        gap = jnp.abs(picked[1:2] - centre)
        scaled = jnp.minimum(gap, cells - gap) / float(LSCALE)
        errors_ref[region : region + 1, :] = picked[0:1] * (1.0 + scaled * scaled)


def solve_kernel(me_ref, pick_ref, errors_ref, values_ref, variance_ref, *refs, masks):
    *blocks_refs, transform_ref, stack_ref, pieces_ref, matrix_refs, left_refs, right_refs, done_refs = refs
    regions, total, _ = transform_ref.shape
    observations = values_ref.shape[1]
    blocks = observations // LANES
    members = blocks_refs[0].shape[1] // (2 * blocks)
    size = pick_ref.shape[2]
    for block in range(blocks):
        lanes = slice(block * LANES, (block + 1) * LANES)
        values = values_ref[:, lanes]
        spread = jnp.sqrt(variance_ref[:, lanes])
        for blocks_ref, mask in zip(blocks_refs, masks, strict=True):
            for number, bits in enumerate(mask):
                source = pl.multiple_of(lax.bitwise_xor(me_ref[0], bits) * members, members)
                equivalents = blocks_ref[number, block * members : (block + 1) * members, :]
                noise = blocks_ref[number, (blocks + block) * members : (blocks + block + 1) * members, :]
                stack_ref[block, pl.ds(source, members), :] = equivalents
                stack_ref[block, pl.ds(total + source, members), :] = values + spread * noise - equivalents
        for number, piece in enumerate(split_two(stack_ref[block])):
            pieces_ref[number * 2 * total : (number + 1) * 2 * total, lanes] = piece
    diagonal = lax.broadcasted_iota(jnp.int32, (size, size), 0) == lax.broadcasted_iota(jnp.int32, (size, size), 1)
    anomalies, innovations = [], []
    for region in range(regions):
        picked = dot(pieces_ref[...], pick_ref[region], ((1,), (0,)), lax.Precision.DEFAULT)
        picked = picked[: 2 * total] + picked[2 * total :]
        equivalents = picked[:total]
        innovations.append(picked[total:])
        anomaly = equivalents - jnp.sum(equivalents, axis=0, keepdims=True) * (1.0 / total)
        anomalies.append(anomaly)
        high, middle, low = split_three(anomaly.T)
        left = jnp.concatenate([high, high, middle, high, low, middle], axis=1)
        high, middle, low = split_three(anomaly)
        right = jnp.concatenate([high, middle, high, low, high, middle], axis=0)
        covariance = dot(left, right, ((1,), (0,)), lax.Precision.DEFAULT) * (1.0 / (total - 1))
        matrix_refs[region][...] = jnp.where(diagonal, covariance + errors_ref[region : region + 1, :], covariance)
    invert_all(matrix_refs, left_refs, right_refs, done_refs)
    for region in range(regions):
        weights = dot_split(innovations[region], matrix_refs[region][...], ((1,), (0,)))
        transform_ref[region, :, :] = dot_split(weights, anomalies[region], ((1,), (1,))) * (1.0 / (total - 1))


def apply_kernel(counts_ref, transform_ref, cells_ref, owned_ref, block_ref, result_ref, staging_ref, out_sem):
    sources, height, _ = cells_ref.shape
    regions, total, _ = transform_ref.shape
    members = total // sources
    tiles = height // members
    for tile in range(tiles):
        lanes = slice(tile * LANES, (tile + 1) * LANES)
        for source in range(sources):
            block_ref[source * members : (source + 1) * members, lanes] = cells_ref[source, tile * members : (tile + 1) * members, :]
    wide = tiles // regions
    for region in range(regions):
        block = block_ref[:, region * wide * LANES : (region + 1) * wide * LANES]
        anomalies = block - jnp.sum(block, axis=0, keepdims=True) * (1.0 / total)
        analysed = block + dot_split(transform_ref[region], anomalies, ((1,), (0,)))
        for place in range(wide):
            result_ref[region * wide + place, :total, :] = analysed[:, place * LANES : (place + 1) * LANES]
    for tile in range(tiles):
        result_ref[tile, total:, :] = jnp.zeros((ROWS, LANES), jnp.float32)

    def window(destination, offset):
        for tile in range(tiles):
            staging_ref[destination, tile * ROWS : (tile + 1) * ROWS, :] = result_ref[tile, pl.ds(offset, CAP), :]
        return offset + counts_ref[destination]

    groups = out_sem.shape[0]
    group = sources // groups
    offset = jnp.int32(0)
    copies = []
    for number in range(groups):
        offset = lax.fori_loop(number * group, (number + 1) * group, window, offset, unroll=True)
        span = slice(number * group, (number + 1) * group)
        copies.append(pltpu.make_async_copy(staging_ref.at[span], owned_ref.at[span], out_sem.at[number]))
        copies[-1].start()
    for copy in copies:
        copy.wait()


def advance_kernel(count_ref, rows_ref, out_ref, staging_ref, out_sem):
    sources, height, _ = rows_ref.shape
    tiles = height // ROWS
    chunks = out_sem.shape[0]
    here = sources // chunks
    width = here * tiles * LANES
    lane = lanes_iota()
    occupied = rows_iota() < count_ref[0]

    def load(source, tile):
        return rows_ref[source, tile * ROWS : (tile + 1) * ROWS, :]

    def out_copy(chunk):
        lanes = pl.ds(pl.multiple_of(chunk * width, width), width)
        return pltpu.make_async_copy(staging_ref.at[chunk], out_ref.at[:, lanes], out_sem.at[chunk])

    def step(chunk, carry):
        start = chunk * here
        before = load(lax.rem(start + sources - 1, sources), tiles - 1)
        before_one = pltpu.roll(before, 1, axis=1)
        before_two = pltpu.roll(before, 2, axis=1)
        current = load(start, 0)
        current_up = pltpu.roll(current, LANES - 1, axis=1)
        for number in range(here * tiles):
            source, tile = divmod(number + 1, tiles)
            after = load(start + source if source < here else lax.rem(start + here, sources), tile)
            after_up = pltpu.roll(after, LANES - 1, axis=1)
            one = pltpu.roll(current, 1, axis=1)
            two = pltpu.roll(current, 2, axis=1)
            left = jnp.where(lane == 0, before_one, one)
            left_two = jnp.where(lane < 2, before_two, two)
            right = jnp.where(lane == LANES - 1, after_up, current_up)
            stepped = current + TIME_STEP * ((right - left_two) * left - current + FORCING)
            staging_ref[chunk, :, number * LANES : (number + 1) * LANES] = jnp.where(occupied, stepped, 0.0)
            before_one, before_two = one, two
            current, current_up = after, after_up
        out_copy(chunk).start()
        return carry

    lax.fori_loop(0, chunks, step, 0)
    for chunk in range(chunks):
        out_copy(chunk).wait()


def whole(space=pltpu.VMEM):
    return pl.BlockSpec(memory_space=space)


def in_vmem(value):
    return pltpu.with_memory_space_constraint(value, pltpu.VMEM)


def per_device(prior_sample_matrix, obs_values, obs_var, measured_indexes, neighbours, perturbation, counts):
    devices = lax.axis_size(AXES)
    depth = lax.axis_size("region")
    device_index = lax.axis_index(AXES)
    me = device_index.reshape(1)
    members, cells = prior_sample_matrix.shape
    total = members * devices
    observations = obs_values.shape[0]
    zones, local = neighbours.shape
    regions = zones // devices
    zone_cells = cells // zones
    blocks = observations // LANES
    share_tiles = cells // devices // LANES
    values = obs_values.reshape(1, observations)
    variance = obs_var.reshape(1, observations)

    def swap(value, bits):
        return lax.ppermute(value, AXES, [(device, device ^ bits) for device in range(devices)])

    exchange = functools.partial(lax.all_to_all, axis_name=AXES, split_axis=0, concat_axis=0, tiled=True)

    pick, errors = pl.pallas_call(
        functools.partial(prepare_kernel, cells=float(cells), zone_cells=zone_cells),
        out_shape=(pltpu.VMEM((regions, observations, local), jnp.bfloat16), pltpu.VMEM((regions, local), jnp.float32)),
        in_specs=[whole(pltpu.SMEM), whole(), whole(), whole()],
        out_specs=(whole(),) * 2,
        name="prepare",
    )(me * regions, neighbours, variance, measured_indexes.reshape(1, observations))

    runs = prior_sample_matrix.reshape(members, cells // LANES, LANES).transpose(1, 0, 2).reshape(-1, LANES)
    height = runs.shape[0]
    tiles = height // LANES
    state, mine = pl.pallas_call(
        functools.partial(forecast_kernel, members=members),
        out_shape=(
            jax.ShapeDtypeStruct((height, LANES), jnp.float32),
            jax.ShapeDtypeStruct((2 * blocks * members, LANES), jnp.float32),
        ),
        in_specs=[whole()] * 3,
        out_specs=(whole(pltpu.HBM), whole()),
        scratch_shapes=[
            pltpu.VMEM((height, LANES), jnp.float32),
            pltpu.VMEM((height, LANES), jnp.float32),
            pltpu.VMEM((max(tiles * (LANES + ROWS), LANES * (tiles + ROWS)), LANES), jnp.float32),
            pltpu.VMEM((2 * blocks, LANES), jnp.int32),
            pltpu.SMEM((2 * blocks, LANES), jnp.int32),
            pltpu.SemaphoreType.DMA,
            pltpu.SemaphoreType.DMA,
        ],
        name="forecast",
    )(measured_indexes.reshape(blocks, LANES), perturbation, runs)

    near = jnp.concatenate([mine[None]] + [swap(mine[None], bits) for bits in range(1, depth)])
    near_mask = list(range(depth))
    far_masks = [[chip * 2 * depth + bits for bits in near_mask] for chip in range(1, devices // (2 * depth))]
    far = []
    for mask in far_masks:
        far.append(swap(near, mask[0]))
    own_cells = exchange(state.reshape(devices, height // devices, LANES))
    partner = swap(near, depth)
    partners = [swap(value, depth) for value in far]
    pieces = [near, partner, *far, *partners]
    masks = [near_mask, [depth ^ bits for bits in near_mask], *far_masks, *[[depth ^ bits for bits in mask] for mask in far_masks]]

    place = in_vmem if sum(piece.size for piece in pieces) * 4 <= VMEM_PIECES else lambda value: value
    transform = pl.pallas_call(
        functools.partial(solve_kernel, masks=masks),
        out_shape=pltpu.VMEM((regions, total, total), jnp.float32),
        in_specs=[whole(pltpu.SMEM)] + [whole()] * (4 + len(pieces)),
        out_specs=whole(),
        scratch_shapes=[
            pltpu.VMEM((blocks, 2 * total, LANES), jnp.float32),
            pltpu.VMEM((4 * total, observations), jnp.bfloat16),
            *invert_scratch(regions, local),
        ],
        name="solve",
    )(me, place(pick), place(errors), values, variance, *map(place, pieces))

    outgoing = pl.pallas_call(
        apply_kernel,
        out_shape=jax.ShapeDtypeStruct((devices, share_tiles * CAP, LANES), jnp.float32),
        in_specs=[whole(pltpu.SMEM), whole(), whole()],
        out_specs=whole(pltpu.HBM),
        scratch_shapes=[
            pltpu.VMEM((total, share_tiles * LANES), jnp.float32),
            pltpu.VMEM((share_tiles, total + ROWS, LANES), jnp.float32),
            pltpu.VMEM((devices, share_tiles * CAP, LANES), jnp.float32),
            pltpu.SemaphoreType.DMA((8,)),
        ],
        name="analyse",
    )(counts, in_vmem(transform), in_vmem(own_cells))
    owned = exchange(outgoing)

    chunks = 4
    return pl.pallas_call(
        advance_kernel,
        out_shape=jax.ShapeDtypeStruct((CAP, cells), jnp.float32),
        in_specs=[whole(pltpu.SMEM), whole()],
        out_specs=whole(pltpu.HBM),
        scratch_shapes=[pltpu.VMEM((chunks, CAP, cells // chunks), jnp.float32), pltpu.SemaphoreType.DMA((chunks,))],
        name="advance",
    )(lax.dynamic_slice_in_dim(counts, device_index, 1, 0), in_vmem(owned))


def solution(mesh):
    rows = P(AXES, None)
    return jax.shard_map(
        per_device, mesh=mesh, in_specs=(rows, P(), P(), P(), P(), rows, P()), out_specs=rows, check_vma=False
    )
```
